32 devices in a mesh: row: 8 (over z, y), col: 4 (over x, core).
Axes of the slice: x: 2, y: 2, z: 4, core: 2. Of those that a mesh axis runs over, the one named last changes fastest.
Arguments:
- rhs: float32 [65536, 256], P(('row', 'col')), may hold values from -6 to 6
- block_target: int32 [512], P(('row', 'col')), may hold values from 0 to 127, as said below
- pivot_inverse: float32 [32768, 1024], P(('row', 'col')), may hold values from -0.25 to 3, as said below
- update_factor: float32 [32768, 1024], P(('row', 'col')), may hold values from -0.1875 to 0.1875
- root_inverse: float32 [4096, 4096], P('row', 'col'), may hold values from -0.25 to 3, as said below
- update_map: int32 [256], P(('row', 'col')), may hold values from 0 to 31
Outputs:
- front_solution: float32 [32768, 256], P(('row', 'col'))
- root_solution: float32 [4096, 256], P(('row', 'col'))
The draws below stay inside these ranges and needn't reach their ends.
Inputs may be any that keep to these rules, and one draw needn't show every extreme that they name: block_target[g] is e * 16 + s: block g goes to the device of row index e in its own column, slot s there. Each device sends exactly 2 blocks to each of 8 devices of its column and none to the others; every slot of every device is filled exactly once. `pivot_inverse`: each device's block of 1024 rows is lower triangular with its diagonal positive. `root_inverse`: lower triangular with its diagonal positive.
All inputs are finite; a program needn't handle non-finite values.
Results may differ from the reference program's by a relative error of at most 0.000073.
Values sent between devices are 32-bit elements; how exact they have to be, the bound alone decides.
A program may use at most 192 MiB of HBM per device.

```python
import math
import jax
import jax.numpy as jnp
import numpy as np
from jax import lax

BLK = 128
NRHS = 256
RB_DEV = 16
CAP = 2
HALF = 1024
ROOT = 4096
N_ROW = 8
N_COL = 4
DEVICES = 32


def draw_block_target(key, part):
    base = jax.random.fold_in(key, 7)
    key_offset, key_local, key_slot = jax.random.split(base, 3)
    senders = RB_DEV // CAP
    offsets = jax.vmap(lambda single: jax.random.permutation(single, N_ROW)[:senders])(jax.random.split(key_offset, N_COL))
    ranks = jax.vmap(lambda single: jax.random.permutation(single, RB_DEV))(jax.random.split(key_local, DEVICES))
    shuffles = jax.vmap(lambda single: jax.random.permutation(single, RB_DEV))(jax.random.split(key_slot, DEVICES))
    device = jnp.arange(DEVICES, dtype=jnp.int32)
    row_index = device // N_COL
    col_index = device % N_COL
    group = ranks // CAP
    chosen = jnp.take_along_axis(offsets[col_index], group, axis=1)
    target_row = (row_index[:, None] + chosen) % N_ROW
    receiver = target_row * N_COL + col_index[:, None]
    slot_place = group * CAP + ranks % CAP
    slot_index = shuffles[receiver, slot_place]
    return (target_row * RB_DEV + slot_index).reshape(-1).astype(jnp.int32)


def lower_factor(key, leading, order):
    key_noise, key_diag = jax.random.split(jax.random.fold_in(key, 11))
    noise = jnp.clip(jax.random.normal(key_noise, (leading, order, order), jnp.float32) / math.sqrt(order), -0.25, 0.25)
    diagonal = jax.random.uniform(key_diag, (leading, order, 1), jnp.float32, 1.0, 2.0)
    rows_iota = jnp.arange(order)[:, None]
    cols_iota = jnp.arange(order)[None, :]
    return jnp.where(rows_iota == cols_iota, diagonal, jnp.where(rows_iota > cols_iota, noise, 0.0))


def draw_pivot_inverse(key, part):
    half = BLK * RB_DEV // 2
    return lower_factor(key, DEVICES, half).reshape(DEVICES * half, half)


def draw_root_inverse(key, part):
    return lower_factor(key, 1, ROOT).reshape(ROOT, ROOT)


def plant(array, rng, low, largest):
    shape = array.shape
    place = [jax.random.randint(jax.random.fold_in(rng, axis), (), 0, shape[axis]) for axis in range(len(shape))]
    array = array.at[tuple(place)].set(low)
    longest = shape.index(max(shape))
    place[longest] = (place[longest] + 1) % shape[longest]
    return array.at[tuple(place)].set(largest)


def block_scale(key, dims, shards, smallest, high):
    gain, own = 1.0, jax.random.fold_in(key, 6)
    for dim, blocks in shards:
        draws = jnp.exp(jax.random.uniform(jax.random.fold_in(own, dim), (blocks,), jnp.float32, smallest / len(shards), high / len(shards)))
        gain = gain * jnp.repeat(draws, dims[dim] // blocks).reshape([-1 if axis == dim else 1 for axis in range(len(dims))])
    return gain


def rank_table(amount, skew):
    weights = [(1 << 20) // math.isqrt(standing ** skew) + 1 for standing in range(1, amount + 1)]
    spread = 1 + sum(weights) // (1 << 30)
    return np.cumsum(np.array([max(1, weight // spread) for weight in weights]))


def ranked(own_key, extent, number_of, lean):
    table = rank_table(number_of, lean)
    lot = jax.random.randint(jax.random.fold_in(own_key, 1), extent, 0, int(table[number_of - 1]))
    standing = jnp.searchsorted(jnp.asarray(table, jnp.int32), lot, side="right")
    return jax.random.permutation(jax.random.fold_in(own_key, 2), number_of)[standing].astype(jnp.int32)


def centred(stream_key, dims, deviation, reach, pieces=(), kind=jnp.bfloat16):
    drawn = deviation * jax.random.normal(stream_key, dims, jnp.float32)
    if pieces:
        drawn = drawn * block_scale(stream_key, dims, pieces, -0.22, 0.18)
    return jnp.clip(drawn, -reach, reach).astype(kind)


def setup_inputs(seed: int = 0) -> dict:
    splits = jax.random.split(jax.random.key(seed), 7)
    rhs = centred(splits[0], (DEVICES * RB_DEV * BLK, NRHS), 1.0, 6.0, ((0, 32),), jnp.float32)
    block_target = draw_block_target(jax.random.fold_in(splits[6], 71), 0)
    pivot_inverse = draw_pivot_inverse(jax.random.fold_in(splits[6], 71), 0)
    update_factor = centred(splits[3], (DEVICES * HALF, HALF), HALF ** -0.5, 0.1875, ((0, 32),), jnp.float32)
    root_inverse = draw_root_inverse(jax.random.fold_in(splits[6], 71), 0)
    update_map = plant(ranked(splits[5], (DEVICES * RB_DEV // 2,), DEVICES, 2), jax.random.fold_in(splits[5], 3), 0, DEVICES - 1).astype(jnp.int32)
    return {"rhs": rhs, "block_target": block_target, "pivot_inverse": pivot_inverse, "update_factor": update_factor, "root_inverse": root_inverse, "update_map": update_map}


def reference(rhs, block_target, pivot_inverse, update_factor, root_inverse, update_map):
    count = DEVICES * RB_DEV
    block_index = jnp.arange(count, dtype=jnp.int32)
    column = (block_index // RB_DEV) % N_COL
    where_to = (((block_target // RB_DEV) * N_COL + column) * RB_DEV + block_target % RB_DEV).astype(jnp.int32)
    blocks = rhs.reshape(count, BLK, NRHS)
    fronts = jnp.zeros_like(blocks).at[where_to].set(blocks).reshape(DEVICES, RB_DEV * BLK, NRHS)
    half = BLK * RB_DEV // 2

    def front_step(operands):
        inverse, factor, front = operands
        solved = jnp.dot(inverse, front[:half], precision=lax.Precision.HIGHEST, preferred_element_type=jnp.float32)
        updated = front[half:] - jnp.dot(factor, solved, precision=lax.Precision.HIGHEST, preferred_element_type=jnp.float32)
        return solved, updated

    solved, updated = lax.map(front_step, (pivot_inverse.reshape(DEVICES, half, half), update_factor.reshape(DEVICES, half, half), fronts))
    root_rhs = jnp.zeros((DEVICES, BLK, NRHS), jnp.float32).at[update_map].add(updated.reshape(-1, BLK, NRHS)).reshape(ROOT, NRHS)
    root_solution = jnp.dot(root_inverse, root_rhs, precision=lax.Precision.HIGHEST, preferred_element_type=jnp.float32)
    return solved.reshape(DEVICES * half, NRHS), root_solution
```

```python
import functools
import jax
import jax.numpy as jnp
from jax import lax
from jax.experimental import pallas as pl
from jax.experimental.pallas import tpu as pltpu
from jax.sharding import PartitionSpec as P

BLK = 128
CAP = 2
LANES = 128
HALF_LANES = 64
TILE = 256
EARLY_ROWS = 64
LAST_ROWS = 32
CORE_SKEW = 2
LEAD = 4
SKEW = 3
Z_SKEW = 4
MESH = pl.DeviceIdType.MESH
VMEM = pl.BlockSpec(memory_space=pltpu.VMEM)
SMEM = pl.BlockSpec(memory_space=pltpu.SMEM)
ANY = pl.BlockSpec(memory_space=pl.ANY)


def split(value):
    high = value.astype(jnp.bfloat16)
    low = (value - high.astype(jnp.float32)).astype(jnp.bfloat16)
    return high, low


def dot3(a_high, a_low, b_high, b_low):
    total = jnp.dot(a_high, b_low, preferred_element_type=jnp.float32)
    total += jnp.dot(a_low, b_high, preferred_element_type=jnp.float32)
    return total + jnp.dot(a_high, b_high, preferred_element_type=jnp.float32)


def run(stages):
    @pl.loop(0, max(offset + count for offset, count, _ in stages))
    def _(t):
        for offset, count, stage in stages:
            i = t - offset

            @pl.when(jnp.logical_and(i >= 0, i < count))
            def _():
                stage(i)


def forward_kernel(
    n_row, n_col, order, target_ref, map_ref, rhs_ref, pivot_hbm, factor_hbm, inverse_hbm,
    solved, out,
    staging, messages, slots, slots_smem, place_ref, weights,
    p_high, p_low, w_high, w_low, x_high, x_low, updated,
    give, got_core, got_x, got_y, mid, up, down, ds, total, got_all, product, got_col,
    weight_sem, slot_sem, send, recv, send_int, recv_int,
    core_send, core_recv, x_send, x_recv, y_send, y_recv, z_send, z_recv, all_send, all_recv,
    col_send, col_recv, *arrived,
):
    n_y = max(1, n_col // 2)
    n_z, n_x = n_row // n_y, n_col // 2
    r, c = lax.axis_index("row"), lax.axis_index("col")
    z, y, x, k = r // n_y, r % n_y, c // 2, c % 2
    held = rhs_ref.shape[0]
    rows = solved.shape[0]
    half = rows // BLK
    parts = len(arrived)
    last = parts - 1
    per_seg = n_row // n_y
    seg = per_seg // 2 * BLK
    out_rows = n_col * BLK
    pair = BLK // 2

    chunk = [LAST_ROWS if q == last else EARLY_ROWS for q in range(parts)]
    steps = [seg // rows_ for rows_ in chunk]

    side = jnp.where(lax.broadcasted_iota(jnp.int32, (1, LANES), 1) < HALF_LANES, 0, 1)

    def swap(value):
        return pltpu.roll(value, HALF_LANES, 1)

    def remote(src, dst, ss, rs, device):
        return pltpu.make_async_remote_copy(
            src_ref=src, dst_ref=dst, send_sem=ss, recv_sem=rs, device_id=device, device_id_type=MESH
        )

    barrier = pltpu.get_barrier_semaphore()
    for d in order:
        pl.semaphore_signal(barrier, inc=1, device_id=(r ^ d, c), device_id_type=MESH)
    for d in range(1, n_col):
        pl.semaphore_signal(barrier, inc=1, device_id=(r, (c + d) % n_col), device_id_type=MESH)

    pivot_copy = pltpu.make_async_copy(pivot_hbm, weights.at[pl.ds(0, rows)], weight_sem.at[0])
    factor_copy = pltpu.make_async_copy(factor_hbm, weights.at[pl.ds(rows, rows)], weight_sem.at[1])
    pivot_copy.start()
    factor_copy.start()

    lane = lax.broadcasted_iota(jnp.int32, (8, 128), 1)
    targets = [target_ref[g] for g in range(held)]

    def chosen(peer):
        first, last_ = jnp.int32(held), jnp.int32(-1)
        slot_first, slot_last = jnp.int32(-1), jnp.int32(-1)
        for g in range(held):
            match = lax.div(targets[g], held) == peer
            fresh = jnp.logical_and(match, last_ < 0)
            first = jnp.where(fresh, g, first)
            slot_first = jnp.where(fresh, lax.rem(targets[g], held), slot_first)
            last_ = jnp.where(match, g, last_)
            slot_last = jnp.where(match, lax.rem(targets[g], held), slot_last)
        message = jnp.where(lane == 0, slot_first, slot_last)
        return jnp.minimum(first, held - 1), jnp.maximum(last_, 0), message

    def stage(first, second, tile):
        cols = slice(tile * LANES, (tile + 1) * LANES)
        a, b = rhs_ref[first, :, cols], rhs_ref[second, :, cols]
        return jnp.where(side == 0, a, swap(b)), jnp.where(side == 0, swap(a), b)

    def data_copy(n, d, q):
        return remote(staging.at[q, n], arrived[q].at[r], send.at[q, n], recv.at[q, n], (r ^ d, c))

    def slot_copy(n, d):
        return remote(messages.at[n], slots.at[r], send_int.at[n], recv_int.at[n], (r ^ d, c))

    picks = []
    for n, d in enumerate(order):
        first, second, messages[n] = chosen(r ^ d)
        picks.append((first, second))
        staging[0, n], staging[1, n] = stage(first, second, 0)
        if n == 0:
            pl.semaphore_wait(barrier, n_row + n_col - 2)
        slot_copy(n, d).start()
        data_copy(n, d, 0).start()
    for n, d in enumerate(order):
        data_copy(n, d, 1).start()
    for tile in range(1, parts // 2):
        for n, d in enumerate(order):
            staging[2 * tile, n], staging[2 * tile + 1, n] = stage(*picks[n], tile)
        for q in (2 * tile, 2 * tile + 1):
            for n, d in enumerate(order):
                data_copy(n, d, q).start()
    first, second, slots[r] = chosen(r)
    for tile in range(parts // 2):
        arrived[2 * tile][r], arrived[2 * tile + 1][r] = stage(first, second, tile)

    pivot_copy.wait()
    factor_copy.wait()
    for start in range(0, rows, TILE):
        band = slice(start, start + TILE)
        p_high[band], p_low[band] = split(weights[band])
    for start in range(0, rows, TILE):
        band = slice(start, start + TILE)
        u_high, u_low = split(weights[rows + start : rows + start + TILE])
        for at in range(0, rows, TILE):
            cols = slice(at, at + TILE)
            w_high[band, cols], w_low[band, cols] = split(
                dot3(u_high[:, at:], u_low[:, at:], p_high[at:, cols], p_low[at:, cols])
            )

    inverse_at = []
    inverse_copies = []
    bands = rows // (2 * seg)
    for e in range(n_y):
        at = (e // bands * out_rows, e % bands * 2 * seg)
        inverse_at.append(at)
        inverse_copies.append(
            pltpu.make_async_copy(
                inverse_hbm.at[:, pl.ds(pl.multiple_of((y - e + n_y) % n_y * (2 * seg), 2 * seg), 2 * seg)],
                weights.at[pl.ds(at[0], out_rows), pl.ds(at[1], 2 * seg)],
                weight_sem.at[e],
            )
        )
    for copy in inverse_copies:
        copy.start()

    for n, d in enumerate(order):
        slot_copy(n, d).wait_recv()
    to_smem = pltpu.make_async_copy(slots, slots_smem, slot_sem)
    to_smem.start()
    to_smem.wait()
    found = [slots_smem[s, 0, rank] for s in range(n_row) for rank in range(CAP)]
    for b in range(held):
        place = jnp.int32(0)
        for j, slot in enumerate(found):
            place = jnp.where(slot == b, j, place)
        place_ref[b] = place

    maps = [map_ref[b] for b in range(half)]
    partner = (r, c - k + (1 - k))

    def twice(q, b):
        place = place_ref[b]
        value = arrived[q][lax.div(place, CAP)]
        return jnp.where(side == lax.rem(place, CAP), value, swap(value))

    def update(q):
        for n, d in enumerate(order):
            data_copy(n, d, q).wait_recv()
        for b in range(half):
            part = slice(b * BLK, (b + 1) * BLK)
            x_high[part], x_low[part] = split(twice(q, b))
        for start in range(0, rows, TILE):
            band = slice(start, start + TILE)
            value = dot3(w_high[band], w_low[band], x_high[...], x_low[...])
            for step in range(TILE // BLK):
                b = start // BLK + step
                updated[b] = twice(q, half + b) - value[step * BLK : (step + 1) * BLK]

    def solve(q):
        for b in range(half):
            part = slice(b * BLK, (b + 1) * BLK)
            x_high[part], x_low[part] = split(jnp.where(side == 0, twice(q, b), twice(q + 1, b)))
        for start in range(0, rows, TILE):
            band, deep = slice(start, start + TILE), slice(0, start + TILE)
            solved[band, q // 2 * LANES : (q // 2 + 1) * LANES] = dot3(
                p_high[band, deep], p_low[band, deep], x_high[deep], x_low[deep]
            )

    def within(q, i):
        return pl.ds(pl.multiple_of(i * chunk[q], chunk[q]), chunk[q])

    def wide(q, i):
        return pl.ds(pl.multiple_of(i * (n_y * chunk[q]), n_y * chunk[q]), n_y * chunk[q])

    def place_of(q, i):
        return pl.ds(pl.multiple_of(q * seg + i * chunk[q], chunk[q]), chunk[q])

    def dense(q, column, i, e):
        at = i * chunk[q]
        block = column * n_row + (y + e) % n_y * per_seg + at // BLK
        wanted = block + side * (per_seg // 2)
        part = pl.ds(pl.multiple_of(at % BLK, chunk[q]), chunk[q])
        value = None
        for b in range(half):
            term = jnp.where(wanted == maps[b], updated[b, part], 0.0)
            value = term if value is None else value + term
        return value

    def core_copy(q, d, part, i):
        return remote(
            give.at[q, d, part], got_core.at[q, d, part], core_send.at[q, d], core_recv.at[q, d, i], partner
        )

    def x_copy(q, d, part, i):
        return remote(
            got_core.at[q, d, part], got_x.at[q, d - 1, part], x_send.at[q, d - 1], x_recv.at[q, d - 1, i],
            (r, (x + d) % n_x * 2 + k),
        )

    def y_device(e):
        return (r - y + (y + e) % n_y, c)

    def slab(q, i, e):
        return pl.ds(pl.multiple_of((i * n_y + e) * chunk[q], chunk[q]), chunk[q])

    def y_copy(q, e, i):
        return remote(
            got_core.at[q, 0, slab(q, i, e)], got_y.at[q, e - 1, within(q, i)],
            y_send.at[q, e - 1], y_recv.at[q, e - 1, i], y_device(e),
        )

    def all_copy(q, e, i):
        return remote(
            total.at[place_of(q, i)], got_all.at[q, e - 1, within(q, i)],
            all_send.at[q, e - 1], all_recv.at[q, e - 1, i], y_device(e),
        )

    def up_copy(q, i, source):
        part = place_of(q, i)
        return remote(source.at[part], up.at[part], z_send.at[q, 0], z_recv.at[q, 0, i], (r + n_y, c))

    def down_copy(q, i, source):
        part = place_of(q, i)
        return remote(source.at[part], down.at[part], z_send.at[q, 1], z_recv.at[q, 1, i], (r - n_y, c))

    def stage_core(q, i):
        for d in range(n_x - 1, -1, -1):
            for e in range(n_y - 1, -1, -1):
                give[q, d, slab(q, i, e)] = dense(q, 2 * ((x + d) % n_x) + (1 - k), i, e)
            core_copy(q, d, wide(q, i), i).start()

    def stage_x(q, i):
        for d in range(n_x - 1, -1, -1):
            values = [dense(q, 2 * ((x + d) % n_x) + k, i, e) for e in range(n_y)]
            core_copy(q, d, wide(q, i), i).wait_recv()
            for e in range(n_y):
                part = slab(q, i, e)
                got_core[q, d, part] = values[e] + got_core[q, d, part]
            if d:
                x_copy(q, d, wide(q, i), i).start()

    def stage_y(q, i):
        for d in range(1, n_x):
            x_copy(q, d, wide(q, i), i).wait_recv()
        for e in range(n_y - 1, -1, -1):
            part = slab(q, i, e)
            value = got_core[q, 0, part]
            for d in range(1, n_x):
                value = value + got_x[q, d - 1, part]
            if e:
                got_core[q, 0, part] = value
                y_copy(q, e, i).start()
            else:
                mid[place_of(q, i)] = value

    def hop(step, q, i):
        part = place_of(q, i)
        for at, landed, summed, go in ((z, up, up, up_copy), (n_z - 1 - z, down, ds, down_copy)):
            @pl.when(at == step)
            def _():
                if step == 0:
                    go(q, i, mid).start()
                else:
                    go(q, i, summed).wait_recv()
                    if step < n_z - 1:
                        summed[part] = mid[part] + landed[part]
                        go(q, i, summed).start()

    def z_first(q, i):
        part = place_of(q, i)
        value = mid[part]
        for e in range(1, n_y):
            y_copy(q, e, i).wait_recv()
            value = value + got_y[q, e - 1, within(q, i)]
        mid[part] = value
        hop(0, q, i)

    def z_last(q, i):
        hop(n_z - 1, q, i)
        part = place_of(q, i)

        @pl.when(z == 0)
        def _():
            total[part] = mid[part] + down[part]

        @pl.when(z == n_z - 1)
        def _():
            total[part] = mid[part] + up[part]

        if n_z > 2:
            @pl.when(jnp.logical_and(z > 0, z < n_z - 1))
            def _():
                total[part] = up[part] + down[part]

        for e in range(1, n_y):
            all_copy(q, e, i).start()

    def multiply(q):
        left = [None] * (out_rows // TILE)
        right = [None] * (out_rows // TILE)
        for e in range(n_y):
            if e:
                for i in range(steps[q]):
                    all_copy(q, e, i).wait_recv()
            b_high, b_low = split(got_all[q, e - 1] if e else total[q * seg : (q + 1) * seg])
            at_row, at_col = inverse_at[e]
            for n in range(out_rows // TILE):
                band = slice(at_row + n * TILE, at_row + (n + 1) * TILE)
                for sums, start in ((left, at_col), (right, at_col + seg)):
                    term = dot3(*split(weights[band, start : start + seg]), b_high, b_low)
                    sums[n] = term if sums[n] is None else sums[n] + term
        for n in range(out_rows // TILE):
            value = jnp.where(side == 0, left[n], right[n])
            value = value + swap(value)
            for step in range(TILE // BLK):
                top = value[step * BLK : step * BLK + pair]
                bottom = value[step * BLK + pair : (step + 1) * BLK]
                product[q, n * (TILE // BLK) + step] = jnp.where(side == 0, top, bottom)
        for d in range(1, n_col):
            col_copy(q, d).start()

    def col_copy(q, d):
        to = (c + d) % n_col
        return remote(product.at[q, to], got_col.at[q, d - 1], col_send.at[q, d - 1], col_recv.at[q, d - 1], (r, to))

    def collect(q):
        sums = []
        for part in (q, q + 1):
            value = product[part, c]
            for d in range(1, n_col):
                col_copy(part, d).wait_recv()
                value = value + got_col[part, d - 1]
            sums.append(value)
        cols = slice(q // 2 * LANES, (q // 2 + 1) * LANES)
        out[:pair, cols] = jnp.where(side == 0, sums[0], swap(sums[1]))
        out[pair:, cols] = jnp.where(side == 0, swap(sums[0]), sums[1])

    def of(fn, *args):
        return functools.partial(fn, *args)

    for q in range(last):
        update(q)
        stages = [
            (0, steps[q], of(stage_core, q)),
            (1, steps[q], of(stage_x, q)),
            (3, steps[q], of(stage_y, q)),
        ]
        if q:
            stages.append((0, steps[q - 1], of(z_first, q - 1)))
        run(stages)
        if q % 2:
            solve(q - 1)

    for copy in inverse_copies:
        copy.wait()
    update(last)
    at = CORE_SKEW + LEAD + SKEW
    stages = [
        (0, steps[last], of(stage_core, last)),
        (CORE_SKEW, steps[last], of(stage_x, last)),
        (CORE_SKEW + LEAD, steps[last], of(stage_y, last)),
        (at, steps[last], of(z_first, last)),
        (0, steps[last - 1], of(z_first, last - 1)),
        (2, 1, lambda i: solve(last - 1)),
    ]
    for step in range(1, n_z - 1):
        stages.append((at + step * SKEW, steps[last], of(hop, step, last)))
    stages.append((at + (n_z - 1) * SKEW, steps[last], of(z_last, last)))
    for q in range(last):
        begin = sum(steps[:q])
        for step in range(1, n_z - 1):
            stages.append((begin + (step - 1) * Z_SKEW, steps[q], of(hop, step, q)))
        stages.append((begin + (n_z - 2) * Z_SKEW, steps[q], of(z_last, q)))
    run(stages)
    for q in range(parts):
        multiply(q)
    for q in range(0, parts, 2):
        collect(q)

    for n, d in enumerate(order):
        slot_copy(n, d).wait_send()
        for q in range(parts):
            data_copy(n, d, q).wait_send()
    for q in range(parts):
        for d in range(1, n_col):
            col_copy(q, d).wait_send()
        everything = pl.ds(0, n_y * seg)
        for d in range(n_x):
            core_copy(q, d, everything, 0).wait_send()
        for d in range(1, n_x):
            x_copy(q, d, everything, 0).wait_send()
        whole = pl.ds(q * seg, seg)
        for e in range(1, n_y):
            remote(
                got_y.at[q, e - 1], got_y.at[q, e - 1], y_send.at[q, e - 1], y_recv.at[q, e - 1, 0], y_device(e)
            ).wait_send()
            remote(
                total.at[whole], got_all.at[q, e - 1], all_send.at[q, e - 1], all_recv.at[q, e - 1, 0], y_device(e)
            ).wait_send()

        @pl.when(z < n_z - 1)
        def _():
            remote(mid.at[whole], up.at[whole], z_send.at[q, 0], z_recv.at[q, 0, 0], (r + n_y, c)).wait_send()

        @pl.when(z > 0)
        def _():
            remote(mid.at[whole], down.at[whole], z_send.at[q, 1], z_recv.at[q, 1, 0], (r - n_y, c)).wait_send()


def shards(rhs, block_target, pivot_inverse, update_factor, root_inverse, update_map):
    n_row, n_col = lax.axis_size("row"), lax.axis_size("col")
    n_y = max(1, n_col // 2)
    n_x = n_col // 2
    width = rhs.shape[1]
    held = rhs.shape[0] // BLK
    rows = pivot_inverse.shape[0]
    parts = width // HALF_LANES
    seg = n_row // n_y // 2 * BLK
    steps = seg // min(EARLY_ROWS, LAST_ROWS)
    f32, bf16 = jnp.float32, jnp.bfloat16
    near = list(range(n_row // 2 - 1, 1, -1))
    cross = list(range(n_row - 1, n_row // 2 - 1, -1))
    order = []
    for n in range(max(len(near), len(cross))):
        order += near[n : n + 1] + cross[n : n + 1]
    order += [1]
    dma = pltpu.SemaphoreType.DMA
    line = pltpu.VMEM((parts * seg, LANES), f32)
    square = pltpu.VMEM((rows, rows), bf16)
    return pl.pallas_call(
        functools.partial(forward_kernel, n_row, n_col, order),
        out_shape=(
            jax.ShapeDtypeStruct((rows, width), f32),
            jax.ShapeDtypeStruct((BLK, width), f32),
        ),
        in_specs=[SMEM, SMEM, VMEM, ANY, ANY, ANY],
        out_specs=(VMEM, VMEM),
        scratch_shapes=[
            pltpu.VMEM((parts, n_row - 1, BLK, LANES), f32),
            pltpu.VMEM((n_row - 1, 8, 128), jnp.int32),
            pltpu.VMEM((n_row, 8, 128), jnp.int32),
            pltpu.SMEM((n_row, 8, 128), jnp.int32),
            pltpu.SMEM((held,), jnp.int32),
            pltpu.VMEM((2 * rows, rows), f32),
        ]
        + [square] * 4
        + [
            pltpu.VMEM((rows, LANES), bf16),
            pltpu.VMEM((rows, LANES), bf16),
            pltpu.VMEM((rows // BLK, BLK, LANES), f32),
            pltpu.VMEM((parts, n_x, n_y * seg, LANES), f32),
            pltpu.VMEM((parts, n_x, n_y * seg, LANES), f32),
            pltpu.VMEM((parts, n_x - 1, n_y * seg, LANES), f32),
            pltpu.VMEM((parts, n_y - 1, seg, LANES), f32),
        ]
        + [line] * 5
        + [
            pltpu.VMEM((parts, n_y - 1, seg, LANES), f32),
            pltpu.VMEM((parts, n_col, BLK // 2, LANES), f32),
            pltpu.VMEM((parts, n_col - 1, BLK // 2, LANES), f32),
            dma((max(2, n_y),)),
            dma(()),
        ]
        + [dma((parts, n_row - 1))] * 2
        + [dma((n_row - 1,))] * 2
        + [
            dma((parts, n_x)),
            dma((parts, n_x, steps)),
            dma((parts, n_x - 1)),
            dma((parts, n_x - 1, steps)),
            dma((parts, n_y - 1)),
            dma((parts, n_y - 1, steps)),
            dma((parts, 2)),
            dma((parts, 2, steps)),
            dma((parts, n_y - 1)),
            dma((parts, n_y - 1, steps)),
            dma((parts, n_col - 1)),
            dma((parts, n_col - 1)),
        ]
        + [pltpu.VMEM((n_row, BLK, LANES), f32)] * parts,
        compiler_params=pltpu.CompilerParams(
            collective_id=0, has_side_effects=True, vmem_limit_bytes=67043328
        ),
        name="forward",
    )(block_target, update_map, rhs.reshape(held, BLK, width), pivot_inverse, update_factor, root_inverse)


def solution(mesh):
    return jax.shard_map(
        shards,
        mesh=mesh,
        in_specs=(
            P(("row", "col"), None),
            P(("row", "col")),
            P(("row", "col"), None),
            P(("row", "col"), None),
            P("row", "col"),
            P(("row", "col")),
        ),
        out_specs=(P(("row", "col"), None), P(("row", "col"), None)),
        check_vma=False,
    )
```

```python
import functools
AHEAD = 2
AFTER = 1
import jax
import jax.numpy as jnp
from jax import lax
from jax.experimental import pallas as pl
from jax.experimental.pallas import tpu as pltpu
from jax.sharding import PartitionSpec as P

BLK = 128
CAP = 2
LANES = 128
HALF_LANES = 64
TILE = 256
EARLY_ROWS = 64
LAST_ROWS = 32
CORE_SKEW = 2
LEAD = 4
SKEW = 3
Z_SKEW = 4
MESH = pl.DeviceIdType.MESH
VMEM = pl.BlockSpec(memory_space=pltpu.VMEM)
SMEM = pl.BlockSpec(memory_space=pltpu.SMEM)
ANY = pl.BlockSpec(memory_space=pl.ANY)


def split(value):
    high = value.astype(jnp.bfloat16)
    low = (value - high.astype(jnp.float32)).astype(jnp.bfloat16)
    return high, low


def dot3(a_high, a_low, b_high, b_low):
    total = jnp.dot(a_high, b_low, preferred_element_type=jnp.float32)
    total += jnp.dot(a_low, b_high, preferred_element_type=jnp.float32)
    return total + jnp.dot(a_high, b_high, preferred_element_type=jnp.float32)


def run(stages):
    @pl.loop(0, max(offset + count for offset, count, _ in stages))
    def _(t):
        for offset, count, stage in stages:
            i = t - offset

            @pl.when(jnp.logical_and(i >= 0, i < count))
            def _():
                stage(i)


def forward_kernel(
    n_row, n_col, order, target_ref, map_ref, rhs_ref, pivot_hbm, factor_hbm, inverse_hbm,
    solved, out,
    staging, messages, slots, slots_smem, place_ref, weights,
    p_high, p_low, w_high, w_low, x_high, x_low, updated,
    give, got_core, got_x, got_y, mid, up, down, ds, total, got_all, product, got_col,
    weight_sem, slot_sem, send, recv, send_int, recv_int,
    core_send, core_recv, x_send, x_recv, y_send, y_recv, z_send, z_recv, all_send, all_recv,
    col_send, col_recv, *arrived,
):
    n_y = max(1, n_col // 2)
    n_z, n_x = n_row // n_y, n_col // 2
    r, c = lax.axis_index("row"), lax.axis_index("col")
    z, y, x, k = r // n_y, r % n_y, c // 2, c % 2
    held = rhs_ref.shape[0]
    rows = solved.shape[0]
    half = rows // BLK
    parts = len(arrived)
    last = parts - 1
    per_seg = n_row // n_y
    seg = per_seg // 2 * BLK
    out_rows = n_col * BLK
    pair = BLK // 2

    chunk = [LAST_ROWS if q == last else EARLY_ROWS for q in range(parts)]
    steps = [seg // rows_ for rows_ in chunk]

    side = jnp.where(lax.broadcasted_iota(jnp.int32, (1, LANES), 1) < HALF_LANES, 0, 1)

    def swap(value):
        return pltpu.roll(value, HALF_LANES, 1)

    def remote(src, dst, ss, rs, device):
        return pltpu.make_async_remote_copy(
            src_ref=src, dst_ref=dst, send_sem=ss, recv_sem=rs, device_id=device, device_id_type=MESH
        )

    barrier = pltpu.get_barrier_semaphore()
    for d in order:
        pl.semaphore_signal(barrier, inc=1, device_id=(r ^ d, c), device_id_type=MESH)
    for d in range(1, n_col):
        pl.semaphore_signal(barrier, inc=1, device_id=(r, (c + d) % n_col), device_id_type=MESH)

    pivot_copy = pltpu.make_async_copy(pivot_hbm, weights.at[pl.ds(0, rows)], weight_sem.at[0])
    factor_copy = pltpu.make_async_copy(factor_hbm, weights.at[pl.ds(rows, rows)], weight_sem.at[1])
    pivot_copy.start()
    factor_copy.start()

    lane = lax.broadcasted_iota(jnp.int32, (8, 128), 1)
    targets = [target_ref[g] for g in range(held)]

    def chosen(peer):
        first, last_ = jnp.int32(held), jnp.int32(-1)
        slot_first, slot_last = jnp.int32(-1), jnp.int32(-1)
        for g in range(held):
            match = lax.div(targets[g], held) == peer
            fresh = jnp.logical_and(match, last_ < 0)
            first = jnp.where(fresh, g, first)
            slot_first = jnp.where(fresh, lax.rem(targets[g], held), slot_first)
            last_ = jnp.where(match, g, last_)
            slot_last = jnp.where(match, lax.rem(targets[g], held), slot_last)
        message = jnp.where(lane == 0, slot_first, slot_last)
        return jnp.minimum(first, held - 1), jnp.maximum(last_, 0), message

    def stage(first, second, tile):
        cols = slice(tile * LANES, (tile + 1) * LANES)
        a, b = rhs_ref[first, :, cols], rhs_ref[second, :, cols]
        return jnp.where(side == 0, a, swap(b)), jnp.where(side == 0, swap(a), b)

    def data_copy(n, d, q):
        return remote(staging.at[q, n], arrived[q].at[r], send.at[q, n], recv.at[q, n], (r ^ d, c))

    def slot_copy(n, d):
        return remote(messages.at[n], slots.at[r], send_int.at[n], recv_int.at[n], (r ^ d, c))

    picks = []
    for n, d in enumerate(order):
        first, second, messages[n] = chosen(r ^ d)
        picks.append((first, second))
        staging[0, n], staging[1, n] = stage(first, second, 0)
        if n == 0:
            pl.semaphore_wait(barrier, n_row + n_col - 2)
        slot_copy(n, d).start()
        data_copy(n, d, 0).start()

    def issue(q):
        if q < parts:
            for n, d in enumerate(order):
                data_copy(n, d, q).start()

    for q in range(1, min(2, AHEAD)):
        issue(q)
    for tile in range(1, parts // 2):
        for n, d in enumerate(order):
            staging[2 * tile, n], staging[2 * tile + 1, n] = stage(*picks[n], tile)
    for q in range(2, AHEAD):
        issue(q)
    first, second, slots[r] = chosen(r)
    for tile in range(parts // 2):
        arrived[2 * tile][r], arrived[2 * tile + 1][r] = stage(first, second, tile)

    pivot_copy.wait()
    factor_copy.wait()
    for start in range(0, rows, TILE):
        band = slice(start, start + TILE)
        p_high[band], p_low[band] = split(weights[band])
    for start in range(0, rows, TILE):
        band = slice(start, start + TILE)
        u_high, u_low = split(weights[rows + start : rows + start + TILE])
        for at in range(0, rows, TILE):
            cols = slice(at, at + TILE)
            w_high[band, cols], w_low[band, cols] = split(
                dot3(u_high[:, at:], u_low[:, at:], p_high[at:, cols], p_low[at:, cols])
            )

    inverse_at = []
    inverse_copies = []
    bands = rows // (2 * seg)
    for e in range(n_y):
        at = (e // bands * out_rows, e % bands * 2 * seg)
        inverse_at.append(at)
        inverse_copies.append(
            pltpu.make_async_copy(
                inverse_hbm.at[:, pl.ds(pl.multiple_of((y - e + n_y) % n_y * (2 * seg), 2 * seg), 2 * seg)],
                weights.at[pl.ds(at[0], out_rows), pl.ds(at[1], 2 * seg)],
                weight_sem.at[e],
            )
        )
    for copy in inverse_copies:
        copy.start()

    for n, d in enumerate(order):
        slot_copy(n, d).wait_recv()
    to_smem = pltpu.make_async_copy(slots, slots_smem, slot_sem)
    to_smem.start()
    to_smem.wait()
    found = [slots_smem[s, 0, rank] for s in range(n_row) for rank in range(CAP)]
    for b in range(held):
        place = jnp.int32(0)
        for j, slot in enumerate(found):
            place = jnp.where(slot == b, j, place)
        place_ref[b] = place

    maps = [map_ref[b] for b in range(half)]
    partner = (r, c - k + (1 - k))

    def twice(q, b):
        place = place_ref[b]
        value = arrived[q][lax.div(place, CAP)]
        return jnp.where(side == lax.rem(place, CAP), value, swap(value))

    def update(q):
        for n, d in enumerate(order):
            data_copy(n, d, q).wait_recv()
        for b in range(half):
            part = slice(b * BLK, (b + 1) * BLK)
            x_high[part], x_low[part] = split(twice(q, b))
        for start in range(0, rows, TILE):
            band = slice(start, start + TILE)
            value = dot3(w_high[band], w_low[band], x_high[...], x_low[...])
            for step in range(TILE // BLK):
                b = start // BLK + step
                updated[b] = twice(q, half + b) - value[step * BLK : (step + 1) * BLK]

    def solve(q):
        for b in range(half):
            part = slice(b * BLK, (b + 1) * BLK)
            x_high[part], x_low[part] = split(jnp.where(side == 0, twice(q, b), twice(q + 1, b)))
        for start in range(0, rows, TILE):
            band, deep = slice(start, start + TILE), slice(0, start + TILE)
            solved[band, q // 2 * LANES : (q // 2 + 1) * LANES] = dot3(
                p_high[band, deep], p_low[band, deep], x_high[deep], x_low[deep]
            )

    def within(q, i):
        return pl.ds(pl.multiple_of(i * chunk[q], chunk[q]), chunk[q])

    def wide(q, i):
        return pl.ds(pl.multiple_of(i * (n_y * chunk[q]), n_y * chunk[q]), n_y * chunk[q])

    def place_of(q, i):
        return pl.ds(pl.multiple_of(q * seg + i * chunk[q], chunk[q]), chunk[q])

    def dense(q, column, i, e):
        at = i * chunk[q]
        block = column * n_row + (y + e) % n_y * per_seg + at // BLK
        wanted = block + side * (per_seg // 2)
        part = pl.ds(pl.multiple_of(at % BLK, chunk[q]), chunk[q])
        value = None
        for b in range(half):
            term = jnp.where(wanted == maps[b], updated[b, part], 0.0)
            value = term if value is None else value + term
        return value

    def core_copy(q, d, part, i):
        return remote(
            give.at[q, d, part], got_core.at[q, d, part], core_send.at[q, d], core_recv.at[q, d, i], partner
        )

    def x_copy(q, d, part, i):
        return remote(
            got_core.at[q, d, part], got_x.at[q, d - 1, part], x_send.at[q, d - 1], x_recv.at[q, d - 1, i],
            (r, (x + d) % n_x * 2 + k),
        )

    def y_device(e):
        return (r - y + (y + e) % n_y, c)

    def slab(q, i, e):
        return pl.ds(pl.multiple_of((i * n_y + e) * chunk[q], chunk[q]), chunk[q])

    def y_copy(q, e, i):
        return remote(
            got_core.at[q, 0, slab(q, i, e)], got_y.at[q, e - 1, within(q, i)],
            y_send.at[q, e - 1], y_recv.at[q, e - 1, i], y_device(e),
        )

    def all_copy(q, e, i):
        return remote(
            total.at[place_of(q, i)], got_all.at[q, e - 1, within(q, i)],
            all_send.at[q, e - 1], all_recv.at[q, e - 1, i], y_device(e),
        )

    def up_copy(q, i, source):
        part = place_of(q, i)
        return remote(source.at[part], up.at[part], z_send.at[q, 0], z_recv.at[q, 0, i], (r + n_y, c))

    def down_copy(q, i, source):
        part = place_of(q, i)
        return remote(source.at[part], down.at[part], z_send.at[q, 1], z_recv.at[q, 1, i], (r - n_y, c))

    def stage_core(q, i):
        for d in range(n_x - 1, -1, -1):
            for e in range(n_y - 1, -1, -1):
                give[q, d, slab(q, i, e)] = dense(q, 2 * ((x + d) % n_x) + (1 - k), i, e)
            core_copy(q, d, wide(q, i), i).start()

    def stage_x(q, i):
        for d in range(n_x - 1, -1, -1):
            values = [dense(q, 2 * ((x + d) % n_x) + k, i, e) for e in range(n_y)]
            core_copy(q, d, wide(q, i), i).wait_recv()
            for e in range(n_y):
                part = slab(q, i, e)
                got_core[q, d, part] = values[e] + got_core[q, d, part]
            if d:
                x_copy(q, d, wide(q, i), i).start()

    def stage_y(q, i):
        for d in range(1, n_x):
            x_copy(q, d, wide(q, i), i).wait_recv()
        for e in range(n_y - 1, -1, -1):
            part = slab(q, i, e)
            value = got_core[q, 0, part]
            for d in range(1, n_x):
                value = value + got_x[q, d - 1, part]
            if e:
                got_core[q, 0, part] = value
                y_copy(q, e, i).start()
            else:
                mid[place_of(q, i)] = value

    def hop(step, q, i):
        part = place_of(q, i)
        for at, landed, summed, go in ((z, up, up, up_copy), (n_z - 1 - z, down, ds, down_copy)):
            @pl.when(at == step)
            def _():
                if step == 0:
                    go(q, i, mid).start()
                else:
                    go(q, i, summed).wait_recv()
                    if step < n_z - 1:
                        summed[part] = mid[part] + landed[part]
                        go(q, i, summed).start()

    def z_first(q, i):
        part = place_of(q, i)
        value = mid[part]
        for e in range(1, n_y):
            y_copy(q, e, i).wait_recv()
            value = value + got_y[q, e - 1, within(q, i)]
        mid[part] = value
        hop(0, q, i)

    def z_last(q, i):
        hop(n_z - 1, q, i)
        part = place_of(q, i)

        @pl.when(z == 0)
        def _():
            total[part] = mid[part] + down[part]

        @pl.when(z == n_z - 1)
        def _():
            total[part] = mid[part] + up[part]

        if n_z > 2:
            @pl.when(jnp.logical_and(z > 0, z < n_z - 1))
            def _():
                total[part] = up[part] + down[part]

        for e in range(1, n_y):
            all_copy(q, e, i).start()

    def multiply(q):
        left = [None] * (out_rows // TILE)
        right = [None] * (out_rows // TILE)
        for e in range(n_y):
            if e:
                for i in range(steps[q]):
                    all_copy(q, e, i).wait_recv()
            b_high, b_low = split(got_all[q, e - 1] if e else total[q * seg : (q + 1) * seg])
            at_row, at_col = inverse_at[e]
            for n in range(out_rows // TILE):
                band = slice(at_row + n * TILE, at_row + (n + 1) * TILE)
                for sums, start in ((left, at_col), (right, at_col + seg)):
                    term = dot3(*split(weights[band, start : start + seg]), b_high, b_low)
                    sums[n] = term if sums[n] is None else sums[n] + term
        for n in range(out_rows // TILE):
            value = jnp.where(side == 0, left[n], right[n])
            value = value + swap(value)
            for step in range(TILE // BLK):
                top = value[step * BLK : step * BLK + pair]
                bottom = value[step * BLK + pair : (step + 1) * BLK]
                product[q, n * (TILE // BLK) + step] = jnp.where(side == 0, top, bottom)
        for d in range(1, n_col):
            col_copy(q, d).start()

    def col_copy(q, d):
        to = (c + d) % n_col
        return remote(product.at[q, to], got_col.at[q, d - 1], col_send.at[q, d - 1], col_recv.at[q, d - 1], (r, to))

    def collect(q):
        sums = []
        for part in (q, q + 1):
            value = product[part, c]
            for d in range(1, n_col):
                col_copy(part, d).wait_recv()
                value = value + got_col[part, d - 1]
            sums.append(value)
        cols = slice(q // 2 * LANES, (q // 2 + 1) * LANES)
        out[:pair, cols] = jnp.where(side == 0, sums[0], swap(sums[1]))
        out[pair:, cols] = jnp.where(side == 0, swap(sums[0]), sums[1])

    def of(fn, *args):
        return functools.partial(fn, *args)

    for q in range(last):
        update(q)
        stages = [
            (0, steps[q], of(stage_core, q)),
            (1, steps[q], of(stage_x, q)),
        ]
        if q:
            stages.append((0, steps[q - 1], of(stage_y, q - 1)))
        if q > 1:
            stages.append((0, steps[q - 2], of(z_first, q - 2)))
        if AFTER == 0: issue(q + AHEAD)
        run(stages)
        if AFTER == 1: issue(q + AHEAD)
        if q % 2:
            solve(q - 1)

    for copy in inverse_copies:
        copy.wait()
    update(last)
    at = CORE_SKEW + LEAD + SKEW
    stages = [
        (0, steps[last], of(stage_core, last)),
        (CORE_SKEW, steps[last], of(stage_x, last)),
        (CORE_SKEW + LEAD, steps[last], of(stage_y, last)),
        (at, steps[last], of(z_first, last)),
        (0, steps[last - 1], of(stage_y, last - 1)),
        (0, steps[last - 2], of(z_first, last - 2)),
        (4, steps[last - 1], of(z_first, last - 1)),
        (2, 1, lambda i: solve(last - 1)),
    ]
    for step in range(1, n_z - 1):
        stages.append((at + step * SKEW, steps[last], of(hop, step, last)))
    stages.append((at + (n_z - 1) * SKEW, steps[last], of(z_last, last)))
    for q in range(last):
        begin = sum(steps[:q])
        for step in range(1, n_z - 1):
            stages.append((begin + (step - 1) * Z_SKEW, steps[q], of(hop, step, q)))
        stages.append((begin + (n_z - 2) * Z_SKEW, steps[q], of(z_last, q)))
    run(stages)
    for q in range(parts):
        multiply(q)
    for q in range(0, parts, 2):
        collect(q)

    for n, d in enumerate(order):
        slot_copy(n, d).wait_send()
        for q in range(parts):
            data_copy(n, d, q).wait_send()
    for q in range(parts):
        for d in range(1, n_col):
            col_copy(q, d).wait_send()
        everything = pl.ds(0, n_y * seg)
        for d in range(n_x):
            core_copy(q, d, everything, 0).wait_send()
        for d in range(1, n_x):
            x_copy(q, d, everything, 0).wait_send()
        whole = pl.ds(q * seg, seg)
        for e in range(1, n_y):
            remote(
                got_y.at[q, e - 1], got_y.at[q, e - 1], y_send.at[q, e - 1], y_recv.at[q, e - 1, 0], y_device(e)
            ).wait_send()
            remote(
                total.at[whole], got_all.at[q, e - 1], all_send.at[q, e - 1], all_recv.at[q, e - 1, 0], y_device(e)
            ).wait_send()

        @pl.when(z < n_z - 1)
        def _():
            remote(mid.at[whole], up.at[whole], z_send.at[q, 0], z_recv.at[q, 0, 0], (r + n_y, c)).wait_send()

        @pl.when(z > 0)
        def _():
            remote(mid.at[whole], down.at[whole], z_send.at[q, 1], z_recv.at[q, 1, 0], (r - n_y, c)).wait_send()


def shards(rhs, block_target, pivot_inverse, update_factor, root_inverse, update_map):
    n_row, n_col = lax.axis_size("row"), lax.axis_size("col")
    n_y = max(1, n_col // 2)
    n_x = n_col // 2
    width = rhs.shape[1]
    held = rhs.shape[0] // BLK
    rows = pivot_inverse.shape[0]
    parts = width // HALF_LANES
    seg = n_row // n_y // 2 * BLK
    steps = seg // min(EARLY_ROWS, LAST_ROWS)
    f32, bf16 = jnp.float32, jnp.bfloat16
    near = list(range(n_row // 2 - 1, 1, -1))
    cross = list(range(n_row - 1, n_row // 2 - 1, -1))
    order = []
    for n in range(max(len(near), len(cross))):
        order += near[n : n + 1] + cross[n : n + 1]
    order += [1]
    dma = pltpu.SemaphoreType.DMA
    line = pltpu.VMEM((parts * seg, LANES), f32)
    square = pltpu.VMEM((rows, rows), bf16)
    return pl.pallas_call(
        functools.partial(forward_kernel, n_row, n_col, order),
        out_shape=(
            jax.ShapeDtypeStruct((rows, width), f32),
            jax.ShapeDtypeStruct((BLK, width), f32),
        ),
        in_specs=[SMEM, SMEM, VMEM, ANY, ANY, ANY],
        out_specs=(VMEM, VMEM),
        scratch_shapes=[
            pltpu.VMEM((parts, n_row - 1, BLK, LANES), f32),
            pltpu.VMEM((n_row - 1, 8, 128), jnp.int32),
            pltpu.VMEM((n_row, 8, 128), jnp.int32),
            pltpu.SMEM((n_row, 8, 128), jnp.int32),
            pltpu.SMEM((held,), jnp.int32),
            pltpu.VMEM((2 * rows, rows), f32),
        ]
        + [square] * 4
        + [
            pltpu.VMEM((rows, LANES), bf16),
            pltpu.VMEM((rows, LANES), bf16),
            pltpu.VMEM((rows // BLK, BLK, LANES), f32),
            pltpu.VMEM((parts, n_x, n_y * seg, LANES), f32),
            pltpu.VMEM((parts, n_x, n_y * seg, LANES), f32),
            pltpu.VMEM((parts, n_x - 1, n_y * seg, LANES), f32),
            pltpu.VMEM((parts, n_y - 1, seg, LANES), f32),
        ]
        + [line] * 5
        + [
            pltpu.VMEM((parts, n_y - 1, seg, LANES), f32),
            pltpu.VMEM((parts, n_col, BLK // 2, LANES), f32),
            pltpu.VMEM((parts, n_col - 1, BLK // 2, LANES), f32),
            dma((max(2, n_y),)),
            dma(()),
        ]
        + [dma((parts, n_row - 1))] * 2
        + [dma((n_row - 1,))] * 2
        + [
            dma((parts, n_x)),
            dma((parts, n_x, steps)),
            dma((parts, n_x - 1)),
            dma((parts, n_x - 1, steps)),
            dma((parts, n_y - 1)),
            dma((parts, n_y - 1, steps)),
            dma((parts, 2)),
            dma((parts, 2, steps)),
            dma((parts, n_y - 1)),
            dma((parts, n_y - 1, steps)),
            dma((parts, n_col - 1)),
            dma((parts, n_col - 1)),
        ]
        + [pltpu.VMEM((n_row, BLK, LANES), f32)] * parts,
        compiler_params=pltpu.CompilerParams(
            collective_id=0, has_side_effects=True, vmem_limit_bytes=67043328
        ),
        name="forward",
    )(block_target, update_map, rhs.reshape(held, BLK, width), pivot_inverse, update_factor, root_inverse)


def solution(mesh):
    return jax.shard_map(
        shards,
        mesh=mesh,
        in_specs=(
            P(("row", "col"), None),
            P(("row", "col")),
            P(("row", "col"), None),
            P(("row", "col"), None),
            P("row", "col"),
            P(("row", "col")),
        ),
        out_specs=(P(("row", "col"), None), P(("row", "col"), None)),
        check_vma=False,
    )
```

```python
import functools
import jax
import jax.numpy as jnp
from jax import lax
from jax.experimental import pallas as pl
from jax.experimental.pallas import tpu as pltpu
from jax.sharding import PartitionSpec as P

BLK = 128
CAP = 2
LANES = 128
HALF_LANES = 64
TILE = 256
EARLY_ROWS = 128
LAST_ROWS = 32
WINDOW = 4
CORE_SKEW = 1
LEAD = 4
SKEW = 3
EARLY_HOPS = 0
SOLVE = 12
LATE = True
OLD = (0, 2, 5)
OLD_SKEW = 4
MESH = pl.DeviceIdType.MESH
VMEM = pl.BlockSpec(memory_space=pltpu.VMEM)
SMEM = pl.BlockSpec(memory_space=pltpu.SMEM)
ANY = pl.BlockSpec(memory_space=pl.ANY)


def split(value):
    high = value.astype(jnp.bfloat16)
    low = (value - high.astype(jnp.float32)).astype(jnp.bfloat16)
    return high, low


def dot3(a_high, a_low, b_high, b_low):
    total = jnp.dot(a_high, b_low, preferred_element_type=jnp.float32)
    total += jnp.dot(a_low, b_high, preferred_element_type=jnp.float32)
    return total + jnp.dot(a_high, b_high, preferred_element_type=jnp.float32)


def run(stages):
    @pl.loop(0, max(offset + count for offset, count, _ in stages))
    def _(t):
        for offset, count, stage in stages:
            i = t - offset

            @pl.when(jnp.logical_and(i >= 0, i < count))
            def _():
                stage(i)


def forward_kernel(
    n_row, n_col, order, target_ref, map_ref, rhs_hbm, pivot_hbm, factor_hbm, inverse_hbm,
    solved_hbm, out,
    rhs_ref, solved, staging, messages, slots, slots_smem, place_ref, weights,
    p_high, p_low, w_high, w_low, x_high, x_low, updated,
    give, got_core, got_x, got_y, got_near, mid, up, down, ds, total, got_all, product, got_col,
    weight_sem, rhs_sem, solved_sem, slot_sem, send, recv, send_int, recv_int,
    core_send, core_recv, x_send, x_recv, y_send, y_recv, near_send, near_recv, z_send, z_recv, all_send, all_recv,
    col_send, col_recv, *arrived,
):
    n_y = max(1, n_col // 2)
    n_z, n_x = n_row // n_y, n_col // 2
    r, c = lax.axis_index("row"), lax.axis_index("col")
    z, y, x, k = r // n_y, r % n_y, c // 2, c % 2
    held = rhs_ref.shape[0]
    rows = solved.shape[0]
    half = rows // BLK
    parts = len(arrived)
    last = parts - 1
    per_seg = n_row // n_y
    seg = per_seg // 2 * BLK
    out_rows = n_col * BLK
    pair = BLK // 2

    chunk = [LAST_ROWS if q == last else EARLY_ROWS for q in range(parts)]
    steps = [seg // rows_ for rows_ in chunk]

    side = jnp.where(lax.broadcasted_iota(jnp.int32, (1, LANES), 1) < HALF_LANES, 0, 1)

    def swap(value):
        return pltpu.roll(value, HALF_LANES, 1)

    def remote(src, dst, ss, rs, device):
        return pltpu.make_async_remote_copy(
            src_ref=src, dst_ref=dst, send_sem=ss, recv_sem=rs, device_id=device, device_id_type=MESH
        )

    rhs_copy = pltpu.make_async_copy(rhs_hbm, rhs_ref, rhs_sem)
    rhs_copy.start()

    def near_device(d, e):
        return (r - y + (y + e) % n_y, (x + d) % n_x * 2 + k)

    near = [(d, e) for d in range(n_x - 1, -1, -1) for e in range(n_y - 1, -1, -1) if d or e]
    diagonal = [(d, e) for d, e in near if d and e]

    barrier = pltpu.get_barrier_semaphore()
    for d in order:
        pl.semaphore_signal(barrier, inc=1, device_id=(r ^ d, c), device_id_type=MESH)
    for d in range(1, n_col):
        pl.semaphore_signal(barrier, inc=1, device_id=(r, (c + d) % n_col), device_id_type=MESH)

    for d, e in diagonal:
        pl.semaphore_signal(barrier, inc=1, device_id=near_device(d, e), device_id_type=MESH)

    pivot_copy = pltpu.make_async_copy(pivot_hbm, weights.at[pl.ds(0, rows)], weight_sem.at[0])
    factor_copy = pltpu.make_async_copy(factor_hbm, weights.at[pl.ds(rows, rows)], weight_sem.at[1])
    pivot_copy.start()
    factor_copy.start()

    lane = lax.broadcasted_iota(jnp.int32, (8, 128), 1)
    targets = [target_ref[g] for g in range(held)]

    def chosen(peer):
        first, last_ = jnp.int32(held), jnp.int32(-1)
        slot_first, slot_last = jnp.int32(-1), jnp.int32(-1)
        for g in range(held):
            match = lax.div(targets[g], held) == peer
            fresh = jnp.logical_and(match, last_ < 0)
            first = jnp.where(fresh, g, first)
            slot_first = jnp.where(fresh, lax.rem(targets[g], held), slot_first)
            last_ = jnp.where(match, g, last_)
            slot_last = jnp.where(match, lax.rem(targets[g], held), slot_last)
        message = jnp.where(lane == 0, slot_first, slot_last)
        return jnp.minimum(first, held - 1), jnp.maximum(last_, 0), message

    def stage(first, second, tile):
        cols = slice(tile * LANES, (tile + 1) * LANES)
        a, b = rhs_ref[first, :, cols], rhs_ref[second, :, cols]
        return jnp.where(side == 0, a, swap(b)), jnp.where(side == 0, swap(a), b)

    def data_copy(n, d, q):
        return remote(staging.at[q, n], arrived[q].at[r], send.at[q, n], recv.at[q, n], (r ^ d, c))

    def slot_copy(n, d):
        return remote(messages.at[n], slots.at[r], send_int.at[n], recv_int.at[n], (r ^ d, c))

    rhs_copy.wait()
    picks = []
    for n, d in enumerate(order):
        first, second, messages[n] = chosen(r ^ d)
        picks.append((first, second))
        staging[0, n], staging[1, n] = stage(first, second, 0)
        if n == 0:
            pl.semaphore_wait(barrier, n_row + n_col - 2 + len(diagonal))
        slot_copy(n, d).start()
        data_copy(n, d, 0).start()
    for tile in range(1, parts // 2):
        for n, d in enumerate(order):
            staging[2 * tile, n], staging[2 * tile + 1, n] = stage(*picks[n], tile)
    queue = [(n, d, q) for q in range(1, parts) for n, d in enumerate(order)]

    def pump(n, d, q):
        data_copy(n, d, q).wait_recv()
        reached = q * len(order) + n + WINDOW
        while queue and queue[0][2] * len(order) + queue[0][0] <= reached:
            data_copy(*queue.pop(0)).start()

    first, second, slots[r] = chosen(r)
    for tile in range(parts // 2):
        arrived[2 * tile][r], arrived[2 * tile + 1][r] = stage(first, second, tile)

    pivot_copy.wait()
    factor_copy.wait()
    for start in range(0, rows, TILE):
        band = slice(start, start + TILE)
        p_high[band], p_low[band] = split(weights[band])
    for start in range(0, rows, TILE):
        band = slice(start, start + TILE)
        u_high, u_low = split(weights[rows + start : rows + start + TILE])
        for at in range(0, rows, TILE):
            cols = slice(at, at + TILE)
            w_high[band, cols], w_low[band, cols] = split(
                dot3(u_high[:, at:], u_low[:, at:], p_high[at:, cols], p_low[at:, cols])
            )

    inverse_at = []
    inverse_copies = []
    bands = rows // (2 * seg)
    for e in range(n_y):
        at = (e // bands * out_rows, e % bands * 2 * seg)
        inverse_at.append(at)
        inverse_copies.append(
            pltpu.make_async_copy(
                inverse_hbm.at[:, pl.ds(pl.multiple_of((y - e + n_y) % n_y * (2 * seg), 2 * seg), 2 * seg)],
                weights.at[pl.ds(at[0], out_rows), pl.ds(at[1], 2 * seg)],
                weight_sem.at[e],
            )
        )
    for copy in inverse_copies:
        copy.start()

    for n, d in enumerate(order):
        slot_copy(n, d).wait_recv()
    to_smem = pltpu.make_async_copy(slots, slots_smem, slot_sem)
    to_smem.start()
    to_smem.wait()
    found = [slots_smem[s, 0, rank] for s in range(n_row) for rank in range(CAP)]
    for b in range(held):
        place = jnp.int32(0)
        for j, slot in enumerate(found):
            place = jnp.where(slot == b, j, place)
        place_ref[b] = place

    maps = [map_ref[b] for b in range(half)]
    partner = (r, c - k + (1 - k))

    def twice(q, b):
        place = place_ref[b]
        value = arrived[q][lax.div(place, CAP)]
        return jnp.where(side == lax.rem(place, CAP), value, swap(value))

    def update(q):
        for b in range(half):
            part = slice(b * BLK, (b + 1) * BLK)
            x_high[part], x_low[part] = split(twice(q, b))
        for start in range(0, rows, TILE):
            band = slice(start, start + TILE)
            value = dot3(w_high[band], w_low[band], x_high[...], x_low[...])
            for step in range(TILE // BLK):
                b = start // BLK + step
                updated[b] = twice(q, half + b) - value[step * BLK : (step + 1) * BLK]

    def solve(q):
        for b in range(half):
            part = slice(b * BLK, (b + 1) * BLK)
            x_high[part], x_low[part] = split(jnp.where(side == 0, twice(q, b), twice(q + 1, b)))
        for start in range(0, rows, TILE):
            band, deep = slice(start, start + TILE), slice(0, start + TILE)
            solved[band, q // 2 * LANES : (q // 2 + 1) * LANES] = dot3(
                p_high[band, deep], p_low[band, deep], x_high[deep], x_low[deep]
            )

    def keep(q):
        cols = pl.ds(q // 2 * LANES, LANES)
        return pltpu.make_async_copy(solved.at[:, cols], solved_hbm.at[:, cols], solved_sem.at[q // 2])

    def within(q, i):
        return pl.ds(pl.multiple_of(i * chunk[q], chunk[q]), chunk[q])

    def wide(q, i):
        return pl.ds(pl.multiple_of(i * (n_y * chunk[q]), n_y * chunk[q]), n_y * chunk[q])

    def place_of(q, i):
        return pl.ds(pl.multiple_of(q * seg + i * chunk[q], chunk[q]), chunk[q])

    def dense(q, column, i, e):
        at = i * chunk[q]
        block = column * n_row + (y + e) % n_y * per_seg + at // BLK
        wanted = block + side * (per_seg // 2)
        part = pl.ds(pl.multiple_of(at % BLK, chunk[q]), chunk[q])
        value = None
        for b in range(half):
            term = jnp.where(wanted == maps[b], updated[b, part], 0.0)
            value = term if value is None else value + term
        return value

    def core_copy(q, d, part, i):
        return remote(
            give.at[q, d, part], got_core.at[q, d, part], core_send.at[q, d], core_recv.at[q, d, i], partner
        )

    def y_device(e):
        return (r - y + (y + e) % n_y, c)

    def slab(q, i, e):
        return pl.ds(pl.multiple_of((i * n_y + e) * chunk[q], chunk[q]), chunk[q])

    def x_copy(q, d, part, i):
        return remote(
            got_core.at[q, d, part], got_x.at[q, d - 1, part], x_send.at[q, d - 1], x_recv.at[q, d - 1, i],
            (r, (x + d) % n_x * 2 + k),
        )

    def y_copy(q, e, i):
        return remote(
            got_core.at[q, 0, slab(q, i, e)], got_y.at[q, e - 1, within(q, i)],
            y_send.at[q, e - 1], y_recv.at[q, e - 1, i], y_device(e),
        )

    def near_copy(q, d, e, i):
        at = d * n_y + e - 1
        return remote(
            got_core.at[q, d, slab(q, i, e)], got_near.at[at, within(q, i)],
            near_send.at[at], near_recv.at[at, i], near_device(d, e),
        )

    def all_copy(q, e, i):
        return remote(
            total.at[place_of(q, i)], got_all.at[q, e - 1, within(q, i)],
            all_send.at[q, e - 1], all_recv.at[q, e - 1, i], y_device(e),
        )

    def up_copy(q, i, source):
        part = place_of(q, i)
        return remote(source.at[part], up.at[part], z_send.at[q, 0], z_recv.at[q, 0, i], (r + n_y, c))

    def down_copy(q, i, source):
        part = place_of(q, i)
        return remote(source.at[part], down.at[part], z_send.at[q, 1], z_recv.at[q, 1, i], (r - n_y, c))

    def stage_core(q, i):
        for d in range(n_x - 1, -1, -1):
            for e in range(n_y - 1, -1, -1):
                give[q, d, slab(q, i, e)] = dense(q, 2 * ((x + d) % n_x) + (1 - k), i, e)
            core_copy(q, d, wide(q, i), i).start()

    def stage_near(q, i):
        for d in range(n_x - 1, -1, -1):
            values = [dense(q, 2 * ((x + d) % n_x) + k, i, e) for e in range(n_y)]
            core_copy(q, d, wide(q, i), i).wait_recv()
            for e in range(n_y - 1, -1, -1):
                part = slab(q, i, e)
                value = values[e] + got_core[q, d, part]
                if d or e:
                    got_core[q, d, part] = value
                    near_copy(q, d, e, i).start()
                else:
                    mid[place_of(q, i)] = value

    def stage_x(q, i):
        for d in range(n_x - 1, -1, -1):
            values = [dense(q, 2 * ((x + d) % n_x) + k, i, e) for e in range(n_y)]
            core_copy(q, d, wide(q, i), i).wait_recv()
            for e in range(n_y):
                part = slab(q, i, e)
                got_core[q, d, part] = values[e] + got_core[q, d, part]
            if d:
                x_copy(q, d, wide(q, i), i).start()

    def stage_y(q, i):
        for d in range(1, n_x):
            x_copy(q, d, wide(q, i), i).wait_recv()
        for e in range(n_y - 1, -1, -1):
            part = slab(q, i, e)
            value = got_core[q, 0, part]
            for d in range(1, n_x):
                value = value + got_x[q, d - 1, part]
            if e:
                got_core[q, 0, part] = value
                y_copy(q, e, i).start()
            else:
                mid[place_of(q, i)] = value

    def hop(step, q, i):
        part = place_of(q, i)
        for at, landed, summed, go in ((z, up, up, up_copy), (n_z - 1 - z, down, ds, down_copy)):
            @pl.when(at == step)
            def _():
                if step == 0:
                    go(q, i, mid).start()
                else:
                    go(q, i, summed).wait_recv()
                    if step < n_z - 1:
                        summed[part] = mid[part] + landed[part]
                        go(q, i, summed).start()

    def z_first(q, i):
        part = place_of(q, i)
        value = mid[part]
        if q == last:
            for d, e in reversed(near):
                near_copy(q, d, e, i).wait_recv()
                value = value + got_near[d * n_y + e - 1, within(q, i)]
        else:
            for e in range(1, n_y):
                y_copy(q, e, i).wait_recv()
                value = value + got_y[q, e - 1, within(q, i)]
        mid[part] = value
        hop(0, q, i)

    def z_last(q, i):
        hop(n_z - 1, q, i)
        part = place_of(q, i)

        @pl.when(z == 0)
        def _():
            total[part] = mid[part] + down[part]

        @pl.when(z == n_z - 1)
        def _():
            total[part] = mid[part] + up[part]

        if n_z > 2:
            @pl.when(jnp.logical_and(z > 0, z < n_z - 1))
            def _():
                total[part] = up[part] + down[part]

        for e in range(1, n_y):
            all_copy(q, e, i).start()

    def multiply(q):
        left = [None] * (out_rows // TILE)
        right = [None] * (out_rows // TILE)
        for e in range(n_y):
            if e:
                for i in range(steps[q]):
                    all_copy(q, e, i).wait_recv()
            b_high, b_low = split(got_all[q, e - 1] if e else total[q * seg : (q + 1) * seg])
            at_row, at_col = inverse_at[e]
            for n in range(out_rows // TILE):
                band = slice(at_row + n * TILE, at_row + (n + 1) * TILE)
                for sums, start in ((left, at_col), (right, at_col + seg)):
                    term = dot3(*split(weights[band, start : start + seg]), b_high, b_low)
                    sums[n] = term if sums[n] is None else sums[n] + term
        for n in range(out_rows // TILE):
            value = jnp.where(side == 0, left[n], right[n])
            value = value + swap(value)
            for step in range(TILE // BLK):
                top = value[step * BLK : step * BLK + pair]
                bottom = value[step * BLK + pair : (step + 1) * BLK]
                product[q, n * (TILE // BLK) + step] = jnp.where(side == 0, top, bottom)
        for d in range(1, n_col):
            col_copy(q, d).start()

    def col_copy(q, d):
        to = (c + d) % n_col
        return remote(product.at[q, to], got_col.at[q, d - 1], col_send.at[q, d - 1], col_recv.at[q, d - 1], (r, to))

    def collect(q):
        sums = []
        for part in (q, q + 1):
            value = product[part, c]
            for d in range(1, n_col):
                col_copy(part, d).wait_recv()
                value = value + got_col[part, d - 1]
            sums.append(value)
        cols = slice(q // 2 * LANES, (q // 2 + 1) * LANES)
        out[:pair, cols] = jnp.where(side == 0, sums[0], swap(sums[1]))
        out[pair:, cols] = jnp.where(side == 0, swap(sums[0]), sums[1])

    def of(fn, *args):
        return functools.partial(fn, *args)

    def each(fn, *args):
        for i in range(steps[args[-1]]):
            fn(*args, i)

    turns = len(order)
    for n, d in enumerate(order):
        pump(n, d, 0)
    for q in range(last):
        update(q)
        for n, d in enumerate(order):
            if n == 0:
                each(stage_core, q)
            if n == 1:
                each(stage_x, q)
            if n == 2 and q % 2:
                solve(q - 1)
                keep(q - 1).start()
            if n == 2 and q:
                each(z_first, q - 1)
            if n == turns - 2:
                each(stage_y, q)
                if q == last - 1:
                    for copy in inverse_copies:
                        copy.wait()
                    for old in range(EARLY_HOPS):
                        each(hop, 1, old)
            pump(n, d, q + 1)

    update(last)
    count = steps[last]
    at = CORE_SKEW + LEAD
    stages = [
        (0, count, of(stage_core, last)),
        (CORE_SKEW, count, of(stage_near, last)),
        (at, count, of(z_first, last)),
    ]
    for step in range(1, n_z - 1):
        stages.append((at + step * SKEW, count, of(hop, step, last)))
    stages.append((at + (n_z - 1) * SKEW, count, of(z_last, last)))
    stages.append((SOLVE, 1, lambda i: solve(last - 1)))
    stages.append((0, steps[last - 1], of(z_first, last - 1)))
    for q in range(last):
        begin = OLD[q]
        for step in range(1, n_z - 1):
            if step > 1 or q >= EARLY_HOPS:
                stages.append((begin + (step - 1) * OLD_SKEW, steps[q], of(hop, step, q)))
        stages.append((begin + (n_z - 2) * OLD_SKEW, steps[q], of(z_last, q)))
        if not LATE:
            stages.append((begin + (n_z - 1) * OLD_SKEW + 1, 1, functools.partial(lambda q, i: multiply(q), q)))
    run(stages)
    keep(last - 1).start()
    for q in range(last if LATE else 0):
        multiply(q)
    multiply(last)
    for q in range(0, parts, 2):
        collect(q)

    for q in range(0, parts, 2):
        keep(q).wait()
    for n, d in enumerate(order):
        slot_copy(n, d).wait_send()
        for q in range(parts):
            data_copy(n, d, q).wait_send()
    for q in range(parts):
        for d in range(1, n_col):
            col_copy(q, d).wait_send()
        everything = pl.ds(0, n_y * seg)
        for d in range(n_x):
            core_copy(q, d, everything, 0).wait_send()
        whole = pl.ds(q * seg, seg)
        if q == last:
            for d, e in near:
                at = d * n_y + e - 1
                remote(
                    got_near.at[at], got_near.at[at], near_send.at[at], near_recv.at[at, 0], near_device(d, e)
                ).wait_send()
        else:
            for d in range(1, n_x):
                x_copy(q, d, everything, 0).wait_send()
            for e in range(1, n_y):
                remote(
                    got_y.at[q, e - 1], got_y.at[q, e - 1], y_send.at[q, e - 1], y_recv.at[q, e - 1, 0], y_device(e)
                ).wait_send()
        for e in range(1, n_y):
            remote(
                total.at[whole], got_all.at[q, e - 1], all_send.at[q, e - 1], all_recv.at[q, e - 1, 0], y_device(e)
            ).wait_send()

        @pl.when(z < n_z - 1)
        def _():
            remote(mid.at[whole], up.at[whole], z_send.at[q, 0], z_recv.at[q, 0, 0], (r + n_y, c)).wait_send()

        @pl.when(z > 0)
        def _():
            remote(mid.at[whole], down.at[whole], z_send.at[q, 1], z_recv.at[q, 1, 0], (r - n_y, c)).wait_send()


def shards(rhs, block_target, pivot_inverse, update_factor, root_inverse, update_map):
    n_row, n_col = lax.axis_size("row"), lax.axis_size("col")
    n_y = max(1, n_col // 2)
    n_x = n_col // 2
    width = rhs.shape[1]
    held = rhs.shape[0] // BLK
    rows = pivot_inverse.shape[0]
    parts = width // HALF_LANES
    seg = n_row // n_y // 2 * BLK
    steps = seg // min(EARLY_ROWS, LAST_ROWS)
    f32, bf16 = jnp.float32, jnp.bfloat16
    near = list(range(n_row // 2 - 1, 1, -1))
    cross = list(range(n_row - 1, n_row // 2 - 1, -1))
    order = []
    for n in range(max(len(near), len(cross))):
        order += near[n : n + 1] + cross[n : n + 1]
    order += [1]
    dma = pltpu.SemaphoreType.DMA
    line = pltpu.VMEM((parts * seg, LANES), f32)
    square = pltpu.VMEM((rows, rows), bf16)
    return pl.pallas_call(
        functools.partial(forward_kernel, n_row, n_col, order),
        out_shape=(
            jax.ShapeDtypeStruct((rows, width), f32),
            jax.ShapeDtypeStruct((BLK, width), f32),
        ),
        in_specs=[SMEM, SMEM, ANY, ANY, ANY, ANY],
        out_specs=(ANY, VMEM),
        scratch_shapes=[
            pltpu.VMEM((held, BLK, width), f32),
            pltpu.VMEM((rows, width), f32),
            pltpu.VMEM((parts, n_row - 1, BLK, LANES), f32),
            pltpu.VMEM((n_row - 1, 8, 128), jnp.int32),
            pltpu.VMEM((n_row, 8, 128), jnp.int32),
            pltpu.SMEM((n_row, 8, 128), jnp.int32),
            pltpu.SMEM((held,), jnp.int32),
            pltpu.VMEM((2 * rows, rows), f32),
        ]
        + [square] * 4
        + [
            pltpu.VMEM((rows, LANES), bf16),
            pltpu.VMEM((rows, LANES), bf16),
            pltpu.VMEM((rows // BLK, BLK, LANES), f32),
            pltpu.VMEM((parts, n_x, n_y * seg, LANES), f32),
            pltpu.VMEM((parts, n_x, n_y * seg, LANES), f32),
            pltpu.VMEM((parts - 1, n_x - 1, n_y * seg, LANES), f32),
            pltpu.VMEM((parts - 1, n_y - 1, seg, LANES), f32),
            pltpu.VMEM((n_x * n_y - 1, seg, LANES), f32),
        ]
        + [line] * 5
        + [
            pltpu.VMEM((parts, n_y - 1, seg, LANES), f32),
            pltpu.VMEM((parts, n_col, BLK // 2, LANES), f32),
            pltpu.VMEM((parts, n_col - 1, BLK // 2, LANES), f32),
            dma((max(2, n_y),)),
            dma(()),
            dma((parts // 2,)),
            dma(()),
        ]
        + [dma((parts, n_row - 1))] * 2
        + [dma((n_row - 1,))] * 2
        + [
            dma((parts, n_x)),
            dma((parts, n_x, steps)),
            dma((parts - 1, n_x - 1)),
            dma((parts - 1, n_x - 1, steps)),
            dma((parts - 1, n_y - 1)),
            dma((parts - 1, n_y - 1, steps)),
            dma((n_x * n_y - 1,)),
            dma((n_x * n_y - 1, steps)),
            dma((parts, 2)),
            dma((parts, 2, steps)),
            dma((parts, n_y - 1)),
            dma((parts, n_y - 1, steps)),
            dma((parts, n_col - 1)),
            dma((parts, n_col - 1)),
        ]
        + [pltpu.VMEM((n_row, BLK, LANES), f32)] * parts,
        compiler_params=pltpu.CompilerParams(
            collective_id=0, has_side_effects=True, vmem_limit_bytes=67043328
        ),
        name="forward",
    )(block_target, update_map, rhs.reshape(held, BLK, width), pivot_inverse, update_factor, root_inverse)


def solution(mesh):
    return jax.shard_map(
        shards,
        mesh=mesh,
        in_specs=(
            P(("row", "col"), None),
            P(("row", "col")),
            P(("row", "col"), None),
            P(("row", "col"), None),
            P("row", "col"),
            P(("row", "col")),
        ),
        out_specs=(P(("row", "col"), None), P(("row", "col"), None)),
        check_vma=False,
    )
```

```python
import functools
import jax
import jax.numpy as jnp
from jax import lax
from jax.experimental import pallas as pl
from jax.experimental.pallas import tpu as pltpu
from jax.sharding import PartitionSpec as P

BLK = 128
CAP = 2
LANES = 128
HALF_LANES = 64
TILE = 256
EARLY_ROWS = 128
LAST_ROWS = 32
WINDOW = 4
CORE_SKEW = 1
LEAD = 4
SKEW = 3
EARLY_HOPS = 0
SOLVE = 12
OLD = (0, 2, 5)
OLD_SKEW = 4
MESH = pl.DeviceIdType.MESH
VMEM = pl.BlockSpec(memory_space=pltpu.VMEM)
SMEM = pl.BlockSpec(memory_space=pltpu.SMEM)
ANY = pl.BlockSpec(memory_space=pl.ANY)


def split(value):
    high = value.astype(jnp.bfloat16)
    low = (value - high.astype(jnp.float32)).astype(jnp.bfloat16)
    return high, low


def dot3(a_high, a_low, b_high, b_low):
    total = jnp.dot(a_high, b_low, preferred_element_type=jnp.float32)
    total += jnp.dot(a_low, b_high, preferred_element_type=jnp.float32)
    return total + jnp.dot(a_high, b_high, preferred_element_type=jnp.float32)


def run(stages):
    @pl.loop(0, max(offset + count for offset, count, _ in stages))
    def _(t):
        for offset, count, stage in stages:
            i = t - offset

            @pl.when(jnp.logical_and(i >= 0, i < count))
            def _():
                stage(i)


def forward_kernel(
    n_row, n_col, order, target_ref, map_ref, rhs_hbm, pivot_hbm, factor_hbm, inverse_hbm,
    solved_hbm, out,
    rhs_ref, solved, staging, messages, slots, slots_smem, place_ref, weights,
    p_high, p_low, w_high, w_low, x_high, x_low, updated,
    give, got_core, got_x, got_y, got_near, mid, up, down, ds, total, got_all, product, got_col,
    weight_sem, rhs_sem, solved_sem, slot_sem, send, recv, send_int, recv_int,
    core_send, core_recv, x_send, x_recv, y_send, y_recv, near_send, near_recv, z_send, z_recv, all_send, all_recv,
    col_send, col_recv, *arrived,
):
    n_y = max(1, n_col // 2)
    n_z, n_x = n_row // n_y, n_col // 2
    r, c = lax.axis_index("row"), lax.axis_index("col")
    z, y, x, k = r // n_y, r % n_y, c // 2, c % 2
    held = rhs_ref.shape[0]
    rows = solved.shape[0]
    half = rows // BLK
    parts = len(arrived)
    last = parts - 1
    per_seg = n_row // n_y
    seg = per_seg // 2 * BLK
    out_rows = n_col * BLK
    pair = BLK // 2

    chunk = [LAST_ROWS if q == last else EARLY_ROWS for q in range(parts)]
    steps = [seg // rows_ for rows_ in chunk]

    side = jnp.where(lax.broadcasted_iota(jnp.int32, (1, LANES), 1) < HALF_LANES, 0, 1)

    def swap(value):
        return pltpu.roll(value, HALF_LANES, 1)

    def remote(src, dst, ss, rs, device):
        return pltpu.make_async_remote_copy(
            src_ref=src, dst_ref=dst, send_sem=ss, recv_sem=rs, device_id=device, device_id_type=MESH
        )

    rhs_copy = pltpu.make_async_copy(rhs_hbm, rhs_ref, rhs_sem)
    rhs_copy.start()

    def near_device(d, e):
        return (r - y + (y + e) % n_y, (x + d) % n_x * 2 + k)

    near = [(d, e) for d in range(n_x - 1, -1, -1) for e in range(n_y - 1, -1, -1) if d or e]
    diagonal = [(d, e) for d, e in near if d and e]

    barrier = pltpu.get_barrier_semaphore()
    for d in order:
        pl.semaphore_signal(barrier, inc=1, device_id=(r ^ d, c), device_id_type=MESH)
    for d in range(1, n_col):
        pl.semaphore_signal(barrier, inc=1, device_id=(r, (c + d) % n_col), device_id_type=MESH)

    for d, e in diagonal:
        pl.semaphore_signal(barrier, inc=1, device_id=near_device(d, e), device_id_type=MESH)

    pivot_copy = pltpu.make_async_copy(pivot_hbm, weights.at[pl.ds(0, rows)], weight_sem.at[0])
    factor_copy = pltpu.make_async_copy(factor_hbm, weights.at[pl.ds(rows, rows)], weight_sem.at[1])
    pivot_copy.start()
    factor_copy.start()

    lane = lax.broadcasted_iota(jnp.int32, (8, 128), 1)
    targets = [target_ref[g] for g in range(held)]

    def chosen(peer):
        first, last_ = jnp.int32(held), jnp.int32(-1)
        slot_first, slot_last = jnp.int32(-1), jnp.int32(-1)
        for g in range(held):
            match = lax.div(targets[g], held) == peer
            fresh = jnp.logical_and(match, last_ < 0)
            first = jnp.where(fresh, g, first)
            slot_first = jnp.where(fresh, lax.rem(targets[g], held), slot_first)
            last_ = jnp.where(match, g, last_)
            slot_last = jnp.where(match, lax.rem(targets[g], held), slot_last)
        message = jnp.where(lane == 0, slot_first, slot_last)
        return jnp.minimum(first, held - 1), jnp.maximum(last_, 0), message

    def stage(first, second, tile):
        cols = slice(tile * LANES, (tile + 1) * LANES)
        a, b = rhs_ref[first, :, cols], rhs_ref[second, :, cols]
        return jnp.where(side == 0, a, swap(b)), jnp.where(side == 0, swap(a), b)

    def data_copy(n, d, q):
        return remote(staging.at[q, n], arrived[q].at[r], send.at[q, n], recv.at[q, n], (r ^ d, c))

    def slot_copy(n, d):
        return remote(messages.at[n], slots.at[r], send_int.at[n], recv_int.at[n], (r ^ d, c))

    rhs_copy.wait()
    picks = []
    for n, d in enumerate(order):
        first, second, messages[n] = chosen(r ^ d)
        picks.append((first, second))
        staging[0, n], staging[1, n] = stage(first, second, 0)
        if n == 0:
            pl.semaphore_wait(barrier, n_row + n_col - 2 + len(diagonal))
        slot_copy(n, d).start()
        data_copy(n, d, 0).start()
    for tile in range(1, parts // 2):
        for n, d in enumerate(order):
            staging[2 * tile, n], staging[2 * tile + 1, n] = stage(*picks[n], tile)
    queue = [(n, d, q) for q in range(1, parts) for n, d in enumerate(order)]

    def pump(n, d, q):
        data_copy(n, d, q).wait_recv()
        reached = q * len(order) + n + WINDOW
        while queue and queue[0][2] * len(order) + queue[0][0] <= reached:
            data_copy(*queue.pop(0)).start()

    first, second, slots[r] = chosen(r)
    for tile in range(parts // 2):
        arrived[2 * tile][r], arrived[2 * tile + 1][r] = stage(first, second, tile)

    pivot_copy.wait()
    factor_copy.wait()
    for start in range(0, rows, TILE):
        band = slice(start, start + TILE)
        p_high[band], p_low[band] = split(weights[band])
    for start in range(0, rows, TILE):
        band = slice(start, start + TILE)
        u_high, u_low = split(weights[rows + start : rows + start + TILE])
        for at in range(0, rows, TILE):
            cols = slice(at, at + TILE)
            w_high[band, cols], w_low[band, cols] = split(
                dot3(u_high[:, at:], u_low[:, at:], p_high[at:, cols], p_low[at:, cols])
            )

    inverse_at = []
    inverse_copies = []
    bands = rows // (2 * seg)
    for e in range(n_y):
        at = (e // bands * out_rows, e % bands * 2 * seg)
        inverse_at.append(at)
        inverse_copies.append(
            pltpu.make_async_copy(
                inverse_hbm.at[:, pl.ds(pl.multiple_of((y - e + n_y) % n_y * (2 * seg), 2 * seg), 2 * seg)],
                weights.at[pl.ds(at[0], out_rows), pl.ds(at[1], 2 * seg)],
                weight_sem.at[e],
            )
        )
    for copy in inverse_copies:
        copy.start()

    for n, d in enumerate(order):
        slot_copy(n, d).wait_recv()
    to_smem = pltpu.make_async_copy(slots, slots_smem, slot_sem)
    to_smem.start()
    to_smem.wait()
    found = [slots_smem[s, 0, rank] for s in range(n_row) for rank in range(CAP)]
    for b in range(held):
        place = jnp.int32(0)
        for j, slot in enumerate(found):
            place = jnp.where(slot == b, j, place)
        place_ref[b] = place

    maps = [map_ref[b] for b in range(half)]
    partner = (r, c - k + (1 - k))

    def twice(q, b):
        place = place_ref[b]
        value = arrived[q][lax.div(place, CAP)]
        return jnp.where(side == lax.rem(place, CAP), value, swap(value))

    def update(q):
        for b in range(half):
            part = slice(b * BLK, (b + 1) * BLK)
            x_high[part], x_low[part] = split(twice(q, b))
        for start in range(0, rows, TILE):
            band = slice(start, start + TILE)
            value = dot3(w_high[band], w_low[band], x_high[...], x_low[...])
            for step in range(TILE // BLK):
                b = start // BLK + step
                updated[b] = twice(q, half + b) - value[step * BLK : (step + 1) * BLK]

    def solve(q):
        for b in range(half):
            part = slice(b * BLK, (b + 1) * BLK)
            x_high[part], x_low[part] = split(jnp.where(side == 0, twice(q, b), twice(q + 1, b)))
        for start in range(0, rows, TILE):
            band, deep = slice(start, start + TILE), slice(0, start + TILE)
            solved[band, q // 2 * LANES : (q // 2 + 1) * LANES] = dot3(
                p_high[band, deep], p_low[band, deep], x_high[deep], x_low[deep]
            )

    def keep(q):
        cols = pl.ds(q // 2 * LANES, LANES)
        return pltpu.make_async_copy(solved.at[:, cols], solved_hbm.at[:, cols], solved_sem.at[q // 2])

    def within(q, i):
        return pl.ds(pl.multiple_of(i * chunk[q], chunk[q]), chunk[q])

    def wide(q, i):
        return pl.ds(pl.multiple_of(i * (n_y * chunk[q]), n_y * chunk[q]), n_y * chunk[q])

    def place_of(q, i):
        return pl.ds(pl.multiple_of(q * seg + i * chunk[q], chunk[q]), chunk[q])

    def dense(q, column, i, e):
        at = i * chunk[q]
        block = column * n_row + (y + e) % n_y * per_seg + at // BLK
        wanted = block + side * (per_seg // 2)
        part = pl.ds(pl.multiple_of(at % BLK, chunk[q]), chunk[q])
        value = None
        for b in range(half):
            term = jnp.where(wanted == maps[b], updated[b, part], 0.0)
            value = term if value is None else value + term
        return value

    def core_copy(q, d, part, i):
        return remote(
            give.at[q, d, part], got_core.at[q, d, part], core_send.at[q, d], core_recv.at[q, d, i], partner
        )

    def y_device(e):
        return (r - y + (y + e) % n_y, c)

    def slab(q, i, e):
        return pl.ds(pl.multiple_of((i * n_y + e) * chunk[q], chunk[q]), chunk[q])

    def x_copy(q, d, part, i):
        return remote(
            got_core.at[q, d, part], got_x.at[q, d - 1, part], x_send.at[q, d - 1], x_recv.at[q, d - 1, i],
            (r, (x + d) % n_x * 2 + k),
        )

    def y_copy(q, e, i):
        return remote(
            got_core.at[q, 0, slab(q, i, e)], got_y.at[q, e - 1, within(q, i)],
            y_send.at[q, e - 1], y_recv.at[q, e - 1, i], y_device(e),
        )

    def near_copy(q, d, e, i):
        at = d * n_y + e - 1
        return remote(
            got_core.at[q, d, slab(q, i, e)], got_near.at[at, within(q, i)],
            near_send.at[at], near_recv.at[at, i], near_device(d, e),
        )

    def all_copy(q, e, i):
        return remote(
            total.at[place_of(q, i)], got_all.at[q, e - 1, within(q, i)],
            all_send.at[q, e - 1], all_recv.at[q, e - 1, i], y_device(e),
        )

    def up_copy(q, i, source):
        part = place_of(q, i)
        return remote(source.at[part], up.at[part], z_send.at[q, 0], z_recv.at[q, 0, i], (r + n_y, c))

    def down_copy(q, i, source):
        part = place_of(q, i)
        return remote(source.at[part], down.at[part], z_send.at[q, 1], z_recv.at[q, 1, i], (r - n_y, c))

    def stage_core(q, i):
        for d in range(n_x - 1, -1, -1):
            for e in range(n_y - 1, -1, -1):
                give[q, d, slab(q, i, e)] = dense(q, 2 * ((x + d) % n_x) + (1 - k), i, e)
            core_copy(q, d, wide(q, i), i).start()

    def stage_near(q, i):
        for d in range(n_x - 1, -1, -1):
            values = [dense(q, 2 * ((x + d) % n_x) + k, i, e) for e in range(n_y)]
            core_copy(q, d, wide(q, i), i).wait_recv()
            for e in range(n_y - 1, -1, -1):
                part = slab(q, i, e)
                value = values[e] + got_core[q, d, part]
                if d or e:
                    got_core[q, d, part] = value
                    near_copy(q, d, e, i).start()
                else:
                    mid[place_of(q, i)] = value

    def stage_x(q, i):
        for d in range(n_x - 1, -1, -1):
            values = [dense(q, 2 * ((x + d) % n_x) + k, i, e) for e in range(n_y)]
            core_copy(q, d, wide(q, i), i).wait_recv()
            for e in range(n_y):
                part = slab(q, i, e)
                got_core[q, d, part] = values[e] + got_core[q, d, part]
            if d:
                x_copy(q, d, wide(q, i), i).start()

    def stage_y(q, i):
        for d in range(1, n_x):
            x_copy(q, d, wide(q, i), i).wait_recv()
        for e in range(n_y - 1, -1, -1):
            part = slab(q, i, e)
            value = got_core[q, 0, part]
            for d in range(1, n_x):
                value = value + got_x[q, d - 1, part]
            if e:
                got_core[q, 0, part] = value
                y_copy(q, e, i).start()
            else:
                mid[place_of(q, i)] = value

    def hop(step, q, i):
        part = place_of(q, i)
        for at, landed, summed, go in ((z, up, up, up_copy), (n_z - 1 - z, down, ds, down_copy)):
            @pl.when(at == step)
            def _():
                if step == 0:
                    go(q, i, mid).start()
                else:
                    go(q, i, summed).wait_recv()
                    if step < n_z - 1:
                        summed[part] = mid[part] + landed[part]
                        go(q, i, summed).start()

    def z_first(q, i):
        part = place_of(q, i)
        value = mid[part]
        if q == last:
            for d, e in reversed(near):
                near_copy(q, d, e, i).wait_recv()
                value = value + got_near[d * n_y + e - 1, within(q, i)]
        else:
            for e in range(1, n_y):
                y_copy(q, e, i).wait_recv()
                value = value + got_y[q, e - 1, within(q, i)]
        mid[part] = value
        hop(0, q, i)

    def z_last(q, i):
        hop(n_z - 1, q, i)
        part = place_of(q, i)

        @pl.when(z == 0)
        def _():
            total[part] = mid[part] + down[part]

        @pl.when(z == n_z - 1)
        def _():
            total[part] = mid[part] + up[part]

        if n_z > 2:
            @pl.when(jnp.logical_and(z > 0, z < n_z - 1))
            def _():
                total[part] = up[part] + down[part]

        for e in range(1, n_y):
            all_copy(q, e, i).start()

    def multiply(q):
        left = [None] * (out_rows // TILE)
        right = [None] * (out_rows // TILE)
        for e in range(n_y):
            if e:
                for i in range(steps[q]):
                    all_copy(q, e, i).wait_recv()
            b_high, b_low = split(got_all[q, e - 1] if e else total[q * seg : (q + 1) * seg])
            at_row, at_col = inverse_at[e]
            for n in range(out_rows // TILE):
                band = slice(at_row + n * TILE, at_row + (n + 1) * TILE)
                for sums, start in ((left, at_col), (right, at_col + seg)):
                    term = dot3(*split(weights[band, start : start + seg]), b_high, b_low)
                    sums[n] = term if sums[n] is None else sums[n] + term
        for n in range(out_rows // TILE):
            value = jnp.where(side == 0, left[n], right[n])
            value = value + swap(value)
            for step in range(TILE // BLK):
                top = value[step * BLK : step * BLK + pair]
                bottom = value[step * BLK + pair : (step + 1) * BLK]
                product[q, n * (TILE // BLK) + step] = jnp.where(side == 0, top, bottom)
        for d in range(1, n_col):
            col_copy(q, d).start()

    def col_copy(q, d):
        to = (c + d) % n_col
        return remote(product.at[q, to], got_col.at[q, d - 1], col_send.at[q, d - 1], col_recv.at[q, d - 1], (r, to))

    def collect(q):
        sums = []
        for part in (q, q + 1):
            value = product[part, c]
            for d in range(1, n_col):
                col_copy(part, d).wait_recv()
                value = value + got_col[part, d - 1]
            sums.append(value)
        cols = slice(q // 2 * LANES, (q // 2 + 1) * LANES)
        out[:pair, cols] = jnp.where(side == 0, sums[0], swap(sums[1]))
        out[pair:, cols] = jnp.where(side == 0, swap(sums[0]), sums[1])

    def of(fn, *args):
        return functools.partial(fn, *args)

    def each(fn, *args):
        for i in range(steps[args[-1]]):
            fn(*args, i)

    turns = len(order)
    for n, d in enumerate(order):
        pump(n, d, 0)
    for q in range(last):
        update(q)
        for n, d in enumerate(order):
            if n == 0:
                each(stage_core, q)
            if n == 1:
                each(stage_x, q)
            if n == 2 and q % 2:
                solve(q - 1)
                keep(q - 1).start()
            if n == 2 and q:
                each(z_first, q - 1)
            if n == turns - 2:
                each(stage_y, q)
                if q == last - 1:
                    for copy in inverse_copies:
                        copy.wait()
                    for old in range(EARLY_HOPS):
                        each(hop, 1, old)
            pump(n, d, q + 1)

    update(last)
    count = steps[last]
    at = CORE_SKEW + LEAD
    stages = [
        (0, count, of(stage_core, last)),
        (CORE_SKEW, count, of(stage_near, last)),
        (at, count, of(z_first, last)),
    ]
    for step in range(1, n_z - 1):
        stages.append((at + step * SKEW, count, of(hop, step, last)))
    stages.append((at + (n_z - 1) * SKEW, count, of(z_last, last)))
    stages.append((SOLVE, 1, lambda i: solve(last - 1)))
    stages.append((0, steps[last - 1], of(z_first, last - 1)))
    for q in range(last):
        begin = OLD[q]
        for step in range(1, n_z - 1):
            if step > 1 or q >= EARLY_HOPS:
                stages.append((begin + (step - 1) * OLD_SKEW, steps[q], of(hop, step, q)))
        stages.append((begin + (n_z - 2) * OLD_SKEW, steps[q], of(z_last, q)))
        if q < last - 1:
            stages.append((14 + 2 * q, 1, functools.partial(lambda q, i: multiply(q), q)))
    run(stages)
    keep(last - 1).start()
    for q in range(last - 1, last):
        multiply(q)
    multiply(last)
    for q in range(0, parts, 2):
        collect(q)

    for q in range(0, parts, 2):
        keep(q).wait()
    for n, d in enumerate(order):
        slot_copy(n, d).wait_send()
        for q in range(parts):
            data_copy(n, d, q).wait_send()
    for q in range(parts):
        for d in range(1, n_col):
            col_copy(q, d).wait_send()
        everything = pl.ds(0, n_y * seg)
        for d in range(n_x):
            core_copy(q, d, everything, 0).wait_send()
        whole = pl.ds(q * seg, seg)
        if q == last:
            for d, e in near:
                at = d * n_y + e - 1
                remote(
                    got_near.at[at], got_near.at[at], near_send.at[at], near_recv.at[at, 0], near_device(d, e)
                ).wait_send()
        else:
            for d in range(1, n_x):
                x_copy(q, d, everything, 0).wait_send()
            for e in range(1, n_y):
                remote(
                    got_y.at[q, e - 1], got_y.at[q, e - 1], y_send.at[q, e - 1], y_recv.at[q, e - 1, 0], y_device(e)
                ).wait_send()
        for e in range(1, n_y):
            remote(
                total.at[whole], got_all.at[q, e - 1], all_send.at[q, e - 1], all_recv.at[q, e - 1, 0], y_device(e)
            ).wait_send()

        @pl.when(z < n_z - 1)
        def _():
            remote(mid.at[whole], up.at[whole], z_send.at[q, 0], z_recv.at[q, 0, 0], (r + n_y, c)).wait_send()

        @pl.when(z > 0)
        def _():
            remote(mid.at[whole], down.at[whole], z_send.at[q, 1], z_recv.at[q, 1, 0], (r - n_y, c)).wait_send()


def place_kernel(solved, root, solved_out, root_out, sem):
    copies = [
        pltpu.make_async_copy(solved, solved_out, sem.at[0]),
        pltpu.make_async_copy(root, root_out, sem.at[1]),
    ]
    for copy in copies:
        copy.start()
    for copy in copies:
        copy.wait()


def shards(rhs, block_target, pivot_inverse, update_factor, root_inverse, update_map):
    n_row, n_col = lax.axis_size("row"), lax.axis_size("col")
    n_y = max(1, n_col // 2)
    n_x = n_col // 2
    width = rhs.shape[1]
    held = rhs.shape[0] // BLK
    rows = pivot_inverse.shape[0]
    parts = width // HALF_LANES
    seg = n_row // n_y // 2 * BLK
    steps = seg // min(EARLY_ROWS, LAST_ROWS)
    f32, bf16 = jnp.float32, jnp.bfloat16
    near = list(range(n_row // 2 - 1, 1, -1))
    cross = list(range(n_row - 1, n_row // 2 - 1, -1))
    order = []
    for n in range(max(len(near), len(cross))):
        order += near[n : n + 1] + cross[n : n + 1]
    order += [1]
    dma = pltpu.SemaphoreType.DMA
    line = pltpu.VMEM((parts * seg, LANES), f32)
    square = pltpu.VMEM((rows, rows), bf16)
    results = pl.pallas_call(
        functools.partial(forward_kernel, n_row, n_col, order),
        out_shape=(
            jax.ShapeDtypeStruct((rows, width), f32),
            jax.ShapeDtypeStruct((BLK, width), f32),
        ),
        in_specs=[SMEM, SMEM, ANY, ANY, ANY, ANY],
        out_specs=(ANY, VMEM),
        scratch_shapes=[
            pltpu.VMEM((held, BLK, width), f32),
            pltpu.VMEM((rows, width), f32),
            pltpu.VMEM((parts, n_row - 1, BLK, LANES), f32),
            pltpu.VMEM((n_row - 1, 8, 128), jnp.int32),
            pltpu.VMEM((n_row, 8, 128), jnp.int32),
            pltpu.SMEM((n_row, 8, 128), jnp.int32),
            pltpu.SMEM((held,), jnp.int32),
            pltpu.VMEM((2 * rows, rows), f32),
        ]
        + [square] * 4
        + [
            pltpu.VMEM((rows, LANES), bf16),
            pltpu.VMEM((rows, LANES), bf16),
            pltpu.VMEM((rows // BLK, BLK, LANES), f32),
            pltpu.VMEM((parts, n_x, n_y * seg, LANES), f32),
            pltpu.VMEM((parts, n_x, n_y * seg, LANES), f32),
            pltpu.VMEM((parts - 1, n_x - 1, n_y * seg, LANES), f32),
            pltpu.VMEM((parts - 1, n_y - 1, seg, LANES), f32),
            pltpu.VMEM((n_x * n_y - 1, seg, LANES), f32),
        ]
        + [line] * 5
        + [
            pltpu.VMEM((parts, n_y - 1, seg, LANES), f32),
            pltpu.VMEM((parts, n_col, BLK // 2, LANES), f32),
            pltpu.VMEM((parts, n_col - 1, BLK // 2, LANES), f32),
            dma((max(2, n_y),)),
            dma(()),
            dma((parts // 2,)),
            dma(()),
        ]
        + [dma((parts, n_row - 1))] * 2
        + [dma((n_row - 1,))] * 2
        + [
            dma((parts, n_x)),
            dma((parts, n_x, steps)),
            dma((parts - 1, n_x - 1)),
            dma((parts - 1, n_x - 1, steps)),
            dma((parts - 1, n_y - 1)),
            dma((parts - 1, n_y - 1, steps)),
            dma((n_x * n_y - 1,)),
            dma((n_x * n_y - 1, steps)),
            dma((parts, 2)),
            dma((parts, 2, steps)),
            dma((parts, n_y - 1)),
            dma((parts, n_y - 1, steps)),
            dma((parts, n_col - 1)),
            dma((parts, n_col - 1)),
        ]
        + [pltpu.VMEM((n_row, BLK, LANES), f32)] * parts,
        compiler_params=pltpu.CompilerParams(
            collective_id=0, has_side_effects=True, vmem_limit_bytes=67043328
        ),
        name="forward",
    )(block_target, update_map, rhs.reshape(held, BLK, width), pivot_inverse, update_factor, root_inverse)
    return pl.pallas_call(
        place_kernel,
        out_shape=tuple(jax.ShapeDtypeStruct(result.shape, f32) for result in results),
        in_specs=[VMEM, VMEM],
        out_specs=(ANY, ANY),
        scratch_shapes=[dma((2,))],
        name="place",
    )(*results)


def solution(mesh):
    return jax.shard_map(
        shards,
        mesh=mesh,
        in_specs=(
            P(("row", "col"), None),
            P(("row", "col")),
            P(("row", "col"), None),
            P(("row", "col"), None),
            P("row", "col"),
            P(("row", "col")),
        ),
        out_specs=(P(("row", "col"), None), P(("row", "col"), None)),
        check_vma=False,
    )
```

```python
import functools
import jax
import jax.numpy as jnp
from jax import lax
from jax.experimental import pallas as pl
from jax.experimental.pallas import tpu as pltpu
from jax.sharding import PartitionSpec as P

BLK = 128
CAP = 2
LANES = 128
HALF_LANES = 64
TILE = 256
EARLY_ROWS = 64
LAST_ROWS = 32
WINDOW = 4
CORE_SKEW = 1
LEAD = 4
SKEW = 3
EARLY_HOPS = 0
SOLVE = 12
OLD = (0, 2, 5)
OLD_SKEW = 4
MESH = pl.DeviceIdType.MESH
VMEM = pl.BlockSpec(memory_space=pltpu.VMEM)
SMEM = pl.BlockSpec(memory_space=pltpu.SMEM)
ANY = pl.BlockSpec(memory_space=pl.ANY)


def split(value):
    high = value.astype(jnp.bfloat16)
    low = (value - high.astype(jnp.float32)).astype(jnp.bfloat16)
    return high, low


def dot3(a_high, a_low, b_high, b_low):
    total = jnp.dot(a_high, b_low, preferred_element_type=jnp.float32)
    total += jnp.dot(a_low, b_high, preferred_element_type=jnp.float32)
    return total + jnp.dot(a_high, b_high, preferred_element_type=jnp.float32)


def run(stages):
    @pl.loop(0, max(offset + count for offset, count, _ in stages))
    def _(t):
        for offset, count, stage in stages:
            i = t - offset

            @pl.when(jnp.logical_and(i >= 0, i < count))
            def _():
                stage(i)


def forward_kernel(
    n_row, n_col, order, target_ref, map_ref, rhs_hbm, pivot_hbm, factor_hbm, inverse_hbm,
    solved_hbm, out,
    rhs_ref, solved, staging, messages, slots, slots_smem, place_ref, weights,
    p_high, p_low, w_high, w_low, x_high, x_low, updated,
    give, got_core, got_x, got_y, got_near, mid, up, down, ds, total, got_all, product, got_col,
    weight_sem, rhs_sem, solved_sem, slot_sem, send, recv, send_int, recv_int,
    core_send, core_recv, x_send, x_recv, y_send, y_recv, near_send, near_recv, z_send, z_recv, all_send, all_recv,
    col_send, col_recv, *arrived,
):
    n_y = max(1, n_col // 2)
    n_z, n_x = n_row // n_y, n_col // 2
    r, c = lax.axis_index("row"), lax.axis_index("col")
    z, y, x, k = r // n_y, r % n_y, c // 2, c % 2
    held = rhs_ref.shape[0]
    rows = solved.shape[0]
    half = rows // BLK
    parts = len(arrived)
    last = parts - 1
    per_seg = n_row // n_y
    seg = per_seg // 2 * BLK
    out_rows = n_col * BLK
    pair = BLK // 2

    chunk = [LAST_ROWS if q == last else EARLY_ROWS for q in range(parts)]
    steps = [seg // rows_ for rows_ in chunk]

    side = jnp.where(lax.broadcasted_iota(jnp.int32, (1, LANES), 1) < HALF_LANES, 0, 1)

    def swap(value):
        return pltpu.roll(value, HALF_LANES, 1)

    def remote(src, dst, ss, rs, device):
        return pltpu.make_async_remote_copy(
            src_ref=src, dst_ref=dst, send_sem=ss, recv_sem=rs, device_id=device, device_id_type=MESH
        )

    rhs_copy = pltpu.make_async_copy(rhs_hbm, rhs_ref, rhs_sem)
    rhs_copy.start()

    def near_device(d, e):
        return (r - y + (y + e) % n_y, (x + d) % n_x * 2 + k)

    near = [(d, e) for d in range(n_x - 1, -1, -1) for e in range(n_y - 1, -1, -1) if d or e]
    diagonal = [(d, e) for d, e in near if d and e]

    barrier = pltpu.get_barrier_semaphore()
    for d in order:
        pl.semaphore_signal(barrier, inc=1, device_id=(r ^ d, c), device_id_type=MESH)
    for d in range(1, n_col):
        pl.semaphore_signal(barrier, inc=1, device_id=(r, (c + d) % n_col), device_id_type=MESH)

    for d, e in diagonal:
        pl.semaphore_signal(barrier, inc=1, device_id=near_device(d, e), device_id_type=MESH)

    pivot_copy = pltpu.make_async_copy(pivot_hbm, weights.at[pl.ds(0, rows)], weight_sem.at[0])
    factor_copy = pltpu.make_async_copy(factor_hbm, weights.at[pl.ds(rows, rows)], weight_sem.at[1])
    pivot_copy.start()
    factor_copy.start()

    lane = lax.broadcasted_iota(jnp.int32, (8, 128), 1)
    targets = [target_ref[g] for g in range(held)]

    def chosen(peer):
        first, last_ = jnp.int32(held), jnp.int32(-1)
        slot_first, slot_last = jnp.int32(-1), jnp.int32(-1)
        for g in range(held):
            match = lax.div(targets[g], held) == peer
            fresh = jnp.logical_and(match, last_ < 0)
            first = jnp.where(fresh, g, first)
            slot_first = jnp.where(fresh, lax.rem(targets[g], held), slot_first)
            last_ = jnp.where(match, g, last_)
            slot_last = jnp.where(match, lax.rem(targets[g], held), slot_last)
        message = jnp.where(lane == 0, slot_first, slot_last)
        return jnp.minimum(first, held - 1), jnp.maximum(last_, 0), message

    def stage(first, second, tile):
        cols = slice(tile * LANES, (tile + 1) * LANES)
        a, b = rhs_ref[first, :, cols], rhs_ref[second, :, cols]
        return jnp.where(side == 0, a, swap(b)), jnp.where(side == 0, swap(a), b)

    def data_copy(n, d, q):
        return remote(staging.at[q, n], arrived[q].at[r], send.at[q, n], recv.at[q, n], (r ^ d, c))

    def slot_copy(n, d):
        return remote(messages.at[n], slots.at[r], send_int.at[n], recv_int.at[n], (r ^ d, c))

    rhs_copy.wait()
    picks = []
    for n, d in enumerate(order):
        first, second, messages[n] = chosen(r ^ d)
        picks.append((first, second))
        staging[0, n], staging[1, n] = stage(first, second, 0)
        if n == 0:
            pl.semaphore_wait(barrier, n_row + n_col - 2 + len(diagonal))
        slot_copy(n, d).start()
        data_copy(n, d, 0).start()
    for tile in range(1, parts // 2):
        for n, d in enumerate(order):
            staging[2 * tile, n], staging[2 * tile + 1, n] = stage(*picks[n], tile)
    queue = [(n, d, q) for q in range(1, parts) for n, d in enumerate(order)]

    def pump(n, d, q):
        data_copy(n, d, q).wait_recv()
        reached = q * len(order) + n + WINDOW
        while queue and queue[0][2] * len(order) + queue[0][0] <= reached:
            data_copy(*queue.pop(0)).start()

    first, second, slots[r] = chosen(r)
    for tile in range(parts // 2):
        arrived[2 * tile][r], arrived[2 * tile + 1][r] = stage(first, second, tile)

    pivot_copy.wait()
    factor_copy.wait()
    for start in range(0, rows, TILE):
        band = slice(start, start + TILE)
        p_high[band], p_low[band] = split(weights[band])
    for start in range(0, rows, TILE):
        band = slice(start, start + TILE)
        u_high, u_low = split(weights[rows + start : rows + start + TILE])
        for at in range(0, rows, TILE):
            cols = slice(at, at + TILE)
            w_high[band, cols], w_low[band, cols] = split(
                dot3(u_high[:, at:], u_low[:, at:], p_high[at:, cols], p_low[at:, cols])
            )

    inverse_at = []
    inverse_copies = []
    bands = rows // (2 * seg)
    for e in range(n_y):
        at = (e // bands * out_rows, e % bands * 2 * seg)
        inverse_at.append(at)
        inverse_copies.append(
            pltpu.make_async_copy(
                inverse_hbm.at[:, pl.ds(pl.multiple_of((y - e + n_y) % n_y * (2 * seg), 2 * seg), 2 * seg)],
                weights.at[pl.ds(at[0], out_rows), pl.ds(at[1], 2 * seg)],
                weight_sem.at[e],
            )
        )
    for copy in inverse_copies:
        copy.start()

    for n, d in enumerate(order):
        slot_copy(n, d).wait_recv()
    to_smem = pltpu.make_async_copy(slots, slots_smem, slot_sem)
    to_smem.start()
    to_smem.wait()
    found = [slots_smem[s, 0, rank] for s in range(n_row) for rank in range(CAP)]
    for b in range(held):
        place = jnp.int32(0)
        for j, slot in enumerate(found):
            place = jnp.where(slot == b, j, place)
        place_ref[b] = place

    maps = [map_ref[b] for b in range(half)]
    partner = (r, c - k + (1 - k))

    def twice(q, b):
        place = place_ref[b]
        value = arrived[q][lax.div(place, CAP)]
        return jnp.where(side == lax.rem(place, CAP), value, swap(value))

    def update(q):
        for b in range(half):
            part = slice(b * BLK, (b + 1) * BLK)
            x_high[part], x_low[part] = split(twice(q, b))
        for start in range(0, rows, TILE):
            band = slice(start, start + TILE)
            value = dot3(w_high[band], w_low[band], x_high[...], x_low[...])
            for step in range(TILE // BLK):
                b = start // BLK + step
                updated[b] = twice(q, half + b) - value[step * BLK : (step + 1) * BLK]

    def solve(q):
        for b in range(half):
            part = slice(b * BLK, (b + 1) * BLK)
            x_high[part], x_low[part] = split(jnp.where(side == 0, twice(q, b), twice(q + 1, b)))
        for start in range(0, rows, TILE):
            band, deep = slice(start, start + TILE), slice(0, start + TILE)
            solved[band, q // 2 * LANES : (q // 2 + 1) * LANES] = dot3(
                p_high[band, deep], p_low[band, deep], x_high[deep], x_low[deep]
            )

    def keep(q):
        cols = pl.ds(q // 2 * LANES, LANES)
        return pltpu.make_async_copy(solved.at[:, cols], solved_hbm.at[:, cols], solved_sem.at[q // 2])

    def within(q, i):
        return pl.ds(pl.multiple_of(i * chunk[q], chunk[q]), chunk[q])

    def wide(q, i):
        return pl.ds(pl.multiple_of(i * (n_y * chunk[q]), n_y * chunk[q]), n_y * chunk[q])

    def place_of(q, i):
        return pl.ds(pl.multiple_of(q * seg + i * chunk[q], chunk[q]), chunk[q])

    def dense(q, column, i, e):
        at = i * chunk[q]
        block = column * n_row + (y + e) % n_y * per_seg + at // BLK
        wanted = block + side * (per_seg // 2)
        part = pl.ds(pl.multiple_of(at % BLK, chunk[q]), chunk[q])
        value = None
        for b in range(half):
            term = jnp.where(wanted == maps[b], updated[b, part], 0.0)
            value = term if value is None else value + term
        return value

    def core_copy(q, d, part, i):
        return remote(
            give.at[q, d, part], got_core.at[q, d, part], core_send.at[q, d], core_recv.at[q, d, i], partner
        )

    def y_device(e):
        return (r - y + (y + e) % n_y, c)

    def slab(q, i, e):
        return pl.ds(pl.multiple_of((i * n_y + e) * chunk[q], chunk[q]), chunk[q])

    def x_copy(q, d, part, i):
        return remote(
            got_core.at[q, d, part], got_x.at[q, d - 1, part], x_send.at[q, d - 1], x_recv.at[q, d - 1, i],
            (r, (x + d) % n_x * 2 + k),
        )

    def y_copy(q, e, i):
        return remote(
            got_core.at[q, 0, slab(q, i, e)], got_y.at[q, e - 1, within(q, i)],
            y_send.at[q, e - 1], y_recv.at[q, e - 1, i], y_device(e),
        )

    def near_copy(q, d, e, i):
        at = d * n_y + e - 1
        return remote(
            got_core.at[q, d, slab(q, i, e)], got_near.at[at, within(q, i)],
            near_send.at[at], near_recv.at[at, i], near_device(d, e),
        )

    def all_copy(q, e, i):
        return remote(
            total.at[place_of(q, i)], got_all.at[q, e - 1, within(q, i)],
            all_send.at[q, e - 1], all_recv.at[q, e - 1, i], y_device(e),
        )

    def up_copy(q, i, source):
        part = place_of(q, i)
        return remote(source.at[part], up.at[part], z_send.at[q, 0], z_recv.at[q, 0, i], (r + n_y, c))

    def down_copy(q, i, source):
        part = place_of(q, i)
        return remote(source.at[part], down.at[part], z_send.at[q, 1], z_recv.at[q, 1, i], (r - n_y, c))

    def stage_core(q, i):
        for d in range(n_x - 1, -1, -1):
            for e in range(n_y - 1, -1, -1):
                give[q, d, slab(q, i, e)] = dense(q, 2 * ((x + d) % n_x) + (1 - k), i, e)
            core_copy(q, d, wide(q, i), i).start()

    def stage_near(q, i):
        for d in range(n_x - 1, -1, -1):
            values = [dense(q, 2 * ((x + d) % n_x) + k, i, e) for e in range(n_y)]
            core_copy(q, d, wide(q, i), i).wait_recv()
            for e in range(n_y - 1, -1, -1):
                part = slab(q, i, e)
                value = values[e] + got_core[q, d, part]
                if d or e:
                    got_core[q, d, part] = value
                    near_copy(q, d, e, i).start()
                else:
                    mid[place_of(q, i)] = value

    def stage_x(q, i):
        for d in range(n_x - 1, -1, -1):
            values = [dense(q, 2 * ((x + d) % n_x) + k, i, e) for e in range(n_y)]
            core_copy(q, d, wide(q, i), i).wait_recv()
            for e in range(n_y):
                part = slab(q, i, e)
                got_core[q, d, part] = values[e] + got_core[q, d, part]
            if d:
                x_copy(q, d, wide(q, i), i).start()

    def stage_y(q, i):
        for d in range(1, n_x):
            x_copy(q, d, wide(q, i), i).wait_recv()
        for e in range(n_y - 1, -1, -1):
            part = slab(q, i, e)
            value = got_core[q, 0, part]
            for d in range(1, n_x):
                value = value + got_x[q, d - 1, part]
            if e:
                got_core[q, 0, part] = value
                y_copy(q, e, i).start()
            else:
                mid[place_of(q, i)] = value

    def hop(step, q, i):
        part = place_of(q, i)
        for at, landed, summed, go in ((z, up, up, up_copy), (n_z - 1 - z, down, ds, down_copy)):
            @pl.when(at == step)
            def _():
                if step == 0:
                    go(q, i, mid).start()
                else:
                    go(q, i, summed).wait_recv()
                    if step < n_z - 1:
                        summed[part] = mid[part] + landed[part]
                        go(q, i, summed).start()

    def z_first(q, i):
        part = place_of(q, i)
        value = mid[part]
        if q == last:
            for d, e in reversed(near):
                near_copy(q, d, e, i).wait_recv()
                value = value + got_near[d * n_y + e - 1, within(q, i)]
        else:
            for e in range(1, n_y):
                y_copy(q, e, i).wait_recv()
                value = value + got_y[q, e - 1, within(q, i)]
        mid[part] = value
        hop(0, q, i)

    def z_last(q, i):
        hop(n_z - 1, q, i)
        part = place_of(q, i)

        @pl.when(z == 0)
        def _():
            total[part] = mid[part] + down[part]

        @pl.when(z == n_z - 1)
        def _():
            total[part] = mid[part] + up[part]

        if n_z > 2:
            @pl.when(jnp.logical_and(z > 0, z < n_z - 1))
            def _():
                total[part] = up[part] + down[part]

        for e in range(1, n_y):
            all_copy(q, e, i).start()

    def multiply(q):
        left = [None] * (out_rows // TILE)
        right = [None] * (out_rows // TILE)
        for e in range(n_y):
            if e:
                for i in range(steps[q]):
                    all_copy(q, e, i).wait_recv()
            b_high, b_low = split(got_all[q, e - 1] if e else total[q * seg : (q + 1) * seg])
            at_row, at_col = inverse_at[e]
            for n in range(out_rows // TILE):
                band = slice(at_row + n * TILE, at_row + (n + 1) * TILE)
                for sums, start in ((left, at_col), (right, at_col + seg)):
                    term = dot3(*split(weights[band, start : start + seg]), b_high, b_low)
                    sums[n] = term if sums[n] is None else sums[n] + term
        for n in range(out_rows // TILE):
            value = jnp.where(side == 0, left[n], right[n])
            value = value + swap(value)
            for step in range(TILE // BLK):
                top = value[step * BLK : step * BLK + pair]
                bottom = value[step * BLK + pair : (step + 1) * BLK]
                product[q, n * (TILE // BLK) + step] = jnp.where(side == 0, top, bottom)
        for d in range(1, n_col):
            col_copy(q, d).start()

    def col_copy(q, d):
        to = (c + d) % n_col
        return remote(product.at[q, to], got_col.at[q, d - 1], col_send.at[q, d - 1], col_recv.at[q, d - 1], (r, to))

    def collect(q):
        sums = []
        for part in (q, q + 1):
            value = product[part, c]
            for d in range(1, n_col):
                col_copy(part, d).wait_recv()
                value = value + got_col[part, d - 1]
            sums.append(value)
        cols = slice(q // 2 * LANES, (q // 2 + 1) * LANES)
        out[:pair, cols] = jnp.where(side == 0, sums[0], swap(sums[1]))
        out[pair:, cols] = jnp.where(side == 0, swap(sums[0]), sums[1])

    def of(fn, *args):
        return functools.partial(fn, *args)

    def each(fn, *args):
        for i in range(steps[args[-1]]):
            fn(*args, i)

    turns = len(order)
    for n, d in enumerate(order):
        pump(n, d, 0)
    for q in range(last):
        update(q)
        for n, d in enumerate(order):
            if n == 0:
                each(stage_core, q)
            if n == 1:
                each(stage_x, q)
            if n == 2 and q % 2:
                solve(q - 1)
                keep(q - 1).start()
            if n == 2 and q:
                each(z_first, q - 1)
            if n == turns - 2:
                each(stage_y, q)
                if q == last - 1:
                    for copy in inverse_copies:
                        copy.wait()
                    for old in range(EARLY_HOPS):
                        each(hop, 1, old)
            pump(n, d, q + 1)

    update(last)
    count = steps[last]
    at = CORE_SKEW + LEAD
    stages = [
        (0, count, of(stage_core, last)),
        (CORE_SKEW, count, of(stage_near, last)),
        (at, count, of(z_first, last)),
    ]
    for step in range(1, n_z - 1):
        stages.append((at + step * SKEW, count, of(hop, step, last)))
    stages.append((at + (n_z - 1) * SKEW, count, of(z_last, last)))
    stages.append((SOLVE, 1, lambda i: solve(last - 1)))
    stages.append((0, steps[last - 1], of(z_first, last - 1)))
    for q in range(last):
        begin = OLD[q]
        for step in range(1, n_z - 1):
            if step > 1 or q >= EARLY_HOPS:
                stages.append((begin + (step - 1) * OLD_SKEW, steps[q], of(hop, step, q)))
        stages.append((begin + (n_z - 2) * OLD_SKEW, steps[q], of(z_last, q)))
        if q < last - 1:
            stages.append((14 + 2 * q, 1, functools.partial(lambda q, i: multiply(q), q)))
    run(stages)
    keep(last - 1).start()
    for q in range(last - 1, last):
        multiply(q)
    multiply(last)
    for q in range(0, parts, 2):
        collect(q)

    for q in range(0, parts, 2):
        keep(q).wait()
    for n, d in enumerate(order):
        slot_copy(n, d).wait_send()
        for q in range(parts):
            data_copy(n, d, q).wait_send()
    for q in range(parts):
        for d in range(1, n_col):
            col_copy(q, d).wait_send()
        everything = pl.ds(0, n_y * seg)
        for d in range(n_x):
            core_copy(q, d, everything, 0).wait_send()
        whole = pl.ds(q * seg, seg)
        if q == last:
            for d, e in near:
                at = d * n_y + e - 1
                remote(
                    got_near.at[at], got_near.at[at], near_send.at[at], near_recv.at[at, 0], near_device(d, e)
                ).wait_send()
        else:
            for d in range(1, n_x):
                x_copy(q, d, everything, 0).wait_send()
            for e in range(1, n_y):
                remote(
                    got_y.at[q, e - 1], got_y.at[q, e - 1], y_send.at[q, e - 1], y_recv.at[q, e - 1, 0], y_device(e)
                ).wait_send()
        for e in range(1, n_y):
            remote(
                total.at[whole], got_all.at[q, e - 1], all_send.at[q, e - 1], all_recv.at[q, e - 1, 0], y_device(e)
            ).wait_send()

        @pl.when(z < n_z - 1)
        def _():
            remote(mid.at[whole], up.at[whole], z_send.at[q, 0], z_recv.at[q, 0, 0], (r + n_y, c)).wait_send()

        @pl.when(z > 0)
        def _():
            remote(mid.at[whole], down.at[whole], z_send.at[q, 1], z_recv.at[q, 1, 0], (r - n_y, c)).wait_send()


def place_kernel(solved, root, solved_out, root_out, sem):
    copies = [
        pltpu.make_async_copy(solved, solved_out, sem.at[0]),
        pltpu.make_async_copy(root, root_out, sem.at[1]),
    ]
    for copy in copies:
        copy.start()
    for copy in copies:
        copy.wait()


def shards(rhs, block_target, pivot_inverse, update_factor, root_inverse, update_map):
    n_row, n_col = lax.axis_size("row"), lax.axis_size("col")
    n_y = max(1, n_col // 2)
    n_x = n_col // 2
    width = rhs.shape[1]
    held = rhs.shape[0] // BLK
    rows = pivot_inverse.shape[0]
    parts = width // HALF_LANES
    seg = n_row // n_y // 2 * BLK
    steps = seg // min(EARLY_ROWS, LAST_ROWS)
    f32, bf16 = jnp.float32, jnp.bfloat16
    near = list(range(n_row // 2 - 1, 1, -1))
    cross = list(range(n_row - 1, n_row // 2 - 1, -1))
    order = []
    for n in range(max(len(near), len(cross))):
        order += near[n : n + 1] + cross[n : n + 1]
    order += [1]
    dma = pltpu.SemaphoreType.DMA
    line = pltpu.VMEM((parts * seg, LANES), f32)
    square = pltpu.VMEM((rows, rows), bf16)
    results = pl.pallas_call(
        functools.partial(forward_kernel, n_row, n_col, order),
        out_shape=(
            jax.ShapeDtypeStruct((rows, width), f32),
            jax.ShapeDtypeStruct((BLK, width), f32),
        ),
        in_specs=[SMEM, SMEM, ANY, ANY, ANY, ANY],
        out_specs=(ANY, VMEM),
        scratch_shapes=[
            pltpu.VMEM((held, BLK, width), f32),
            pltpu.VMEM((rows, width), f32),
            pltpu.VMEM((parts, n_row - 1, BLK, LANES), f32),
            pltpu.VMEM((n_row - 1, 8, 128), jnp.int32),
            pltpu.VMEM((n_row, 8, 128), jnp.int32),
            pltpu.SMEM((n_row, 8, 128), jnp.int32),
            pltpu.SMEM((held,), jnp.int32),
            pltpu.VMEM((2 * rows, rows), f32),
        ]
        + [square] * 4
        + [
            pltpu.VMEM((rows, LANES), bf16),
            pltpu.VMEM((rows, LANES), bf16),
            pltpu.VMEM((rows // BLK, BLK, LANES), f32),
            pltpu.VMEM((parts, n_x, n_y * seg, LANES), f32),
            pltpu.VMEM((parts, n_x, n_y * seg, LANES), f32),
            pltpu.VMEM((parts - 1, n_x - 1, n_y * seg, LANES), f32),
            pltpu.VMEM((parts - 1, n_y - 1, seg, LANES), f32),
            pltpu.VMEM((n_x * n_y - 1, seg, LANES), f32),
        ]
        + [line] * 5
        + [
            pltpu.VMEM((parts, n_y - 1, seg, LANES), f32),
            pltpu.VMEM((parts, n_col, BLK // 2, LANES), f32),
            pltpu.VMEM((parts, n_col - 1, BLK // 2, LANES), f32),
            dma((max(2, n_y),)),
            dma(()),
            dma((parts // 2,)),
            dma(()),
        ]
        + [dma((parts, n_row - 1))] * 2
        + [dma((n_row - 1,))] * 2
        + [
            dma((parts, n_x)),
            dma((parts, n_x, steps)),
            dma((parts - 1, n_x - 1)),
            dma((parts - 1, n_x - 1, steps)),
            dma((parts - 1, n_y - 1)),
            dma((parts - 1, n_y - 1, steps)),
            dma((n_x * n_y - 1,)),
            dma((n_x * n_y - 1, steps)),
            dma((parts, 2)),
            dma((parts, 2, steps)),
            dma((parts, n_y - 1)),
            dma((parts, n_y - 1, steps)),
            dma((parts, n_col - 1)),
            dma((parts, n_col - 1)),
        ]
        + [pltpu.VMEM((n_row, BLK, LANES), f32)] * parts,
        compiler_params=pltpu.CompilerParams(
            collective_id=0, has_side_effects=True, vmem_limit_bytes=67043328
        ),
        name="forward",
    )(block_target, update_map, rhs.reshape(held, BLK, width), pivot_inverse, update_factor, root_inverse)
    return pl.pallas_call(
        place_kernel,
        out_shape=tuple(jax.ShapeDtypeStruct(result.shape, f32) for result in results),
        in_specs=[VMEM, VMEM],
        out_specs=(ANY, ANY),
        scratch_shapes=[dma((2,))],
        name="place",
    )(*results)


def solution(mesh):
    return jax.shard_map(
        shards,
        mesh=mesh,
        in_specs=(
            P(("row", "col"), None),
            P(("row", "col")),
            P(("row", "col"), None),
            P(("row", "col"), None),
            P("row", "col"),
            P(("row", "col")),
        ),
        out_specs=(P(("row", "col"), None), P(("row", "col"), None)),
        check_vma=False,
    )
```
